32 devices in a mesh: shard: 8 (over y, x, core), dp: 4 (over z).
Axes of the slice: x: 2, y: 2, z: 4, core: 2. Of those that a mesh axis runs over, the one named last changes fastest.
Arguments:
- grad: float32 [288, 128, 4096], P('shard', 'dp'), may hold values from -252 to 252
- param: bfloat16 [288, 128, 4096], P('shard', 'dp'), may hold values from -0.119628906 to 0.119628906
- row_state: float32 [288, 128], P('shard', 'dp'), may hold values from 0.3 to 27
- col_state: float32 [3, 4096], replicated, may hold values from 0.002 to 400
- block_start: int32 [8], replicated, may hold values from 0 to 143, as said below
- block_matrix: int32 [144], replicated, may hold values from 0 to 2, as said below
- step: int32 [1], replicated, may hold values from 2 to 11
Outputs:
- new_params: bfloat16 [18432, 4096], P(None, 'shard')
- new_row_state: float32 [288, 128], P('shard', 'dp')
- new_col_state: float32 [3, 4096], replicated
The draws below stay inside these ranges and needn't reach their ends.
Inputs may be any that keep to these rules, and one draw needn't show every extreme that they name: block_start rises from 0 at index 0; every shard index owns between 1 and 36 consecutive global blocks, held in its first slots, and some index owns exactly 36; slots past a device's owned count hold values that no output reads. `block_matrix`: ids 0 and 1 each label 4096 / 128 blocks and id 2 labels 10240 / 128 blocks, in any order.
All inputs are finite; a program needn't handle non-finite values.
Results may differ from the reference program's by a relative error of at most 0.0004.
Values may be sent and summed in bfloat16 or wider, within the bound.
A program may use at most 192 MiB of HBM per device.

```python
import math
import jax
import jax.numpy as jnp
from jax import lax

D = 4096
FF = 10240
BLOCK = 128
MATS = 3
NB = 144
CAP = 36
N_SHARD = 8


def draw_grad(key, part):
    noise_key, row_key, col_key = jax.random.split(jax.random.fold_in(key, 11), 3)
    slot_total = N_SHARD * CAP
    draw_base = jnp.clip(jax.random.normal(noise_key, (slot_total, BLOCK, D), jnp.float32), -4.0, 4.0)
    row_scale = jnp.exp(jax.random.uniform(row_key, (slot_total, BLOCK), jnp.float32, math.log(0.3), math.log(3.0)))
    col_scale = jnp.exp(jax.random.uniform(col_key, (D,), jnp.float32, math.log(0.3), math.log(3.0)))
    position = jnp.arange(slot_total, dtype=jnp.float32) / max(slot_total - 1, 1)
    ramp_scale = 1.0 + 2.0 * position
    return draw_base * (row_scale * ramp_scale[:, None])[:, :, None] * col_scale[None, None, :]


def draw_row_state(key, part):
    slot_total = N_SHARD * CAP
    state_key = jax.random.fold_in(key, 23)
    position = jnp.arange(slot_total, dtype=jnp.float32) / max(slot_total - 1, 1)
    values = jnp.exp(jax.random.uniform(state_key, (slot_total, BLOCK), jnp.float32, math.log(0.3), math.log(3.0)))
    ramp_scale = 1.0 + 2.0 * position
    return values * ramp_scale[:, None]


def draw_col_state(key, part):
    state_key = jax.random.fold_in(key, 37)
    lowest = jnp.array([0.002, 64.0, 0.002], jnp.float32)
    factor = jnp.exp(jax.random.uniform(state_key, (MATS, D), jnp.float32, 0.0, math.log(4.0)))
    return lowest[:, None] * factor


def draw_block_matrix(key, part):
    order_key = jax.random.fold_in(key, 41)
    block_index = jnp.arange(NB, dtype=jnp.int32)
    first_end = D // BLOCK
    second_end = 2 * (D // BLOCK)
    labels = (block_index >= first_end).astype(jnp.int32) + (block_index >= second_end).astype(jnp.int32)
    return jax.random.permutation(order_key, labels).astype(jnp.int32)


def draw_block_start(key, part):
    busy_key, move_key = jax.random.split(jax.random.fold_in(key, 53))
    busy_device = jax.random.randint(busy_key, (), 0, N_SHARD - 1)
    last_device = N_SHARD - 1
    rest_blocks = NB - CAP - 1
    base_count = rest_blocks // (N_SHARD - 2)
    extra_count = rest_blocks % (N_SHARD - 2)
    device_ids = jnp.arange(N_SHARD, dtype=jnp.int32)
    position_rank = device_ids - (device_ids > busy_device).astype(jnp.int32)
    spread_count = base_count + (position_rank < extra_count).astype(jnp.int32)
    counts = jnp.where(device_ids == busy_device, CAP, jnp.where(device_ids == last_device, 1, spread_count)).astype(jnp.int32)

    def move(turn, counts):
        turn_key = jax.random.fold_in(move_key, turn)
        pair_key, amount_key = jax.random.split(turn_key)
        ends_pair = jax.random.randint(pair_key, (2,), 0, N_SHARD)
        source = ends_pair[0]
        target = ends_pair[1]
        wanted = jax.random.randint(amount_key, (), 0, CAP)
        usable = (source != busy_device) & (target != busy_device) & (source != target) & (source != last_device) & (target != last_device)
        amount = jnp.minimum(jnp.minimum(wanted, counts[source] - 1), CAP - counts[target])
        amount = jnp.where(usable, jnp.maximum(amount, 0), 0).astype(jnp.int32)
        return counts.at[source].add(-amount).at[target].add(amount)
    counts = lax.fori_loop(0, 4 * N_SHARD, move, counts)
    return (jnp.cumsum(counts) - counts).astype(jnp.int32)


def levels(stream_key, dims, pieces, least, largest):
    gain = 1.0
    for axis_at, parts in pieces:
        draws = jax.random.uniform(jax.random.fold_in(jax.random.fold_in(stream_key, 6), axis_at), (parts,), jnp.float32, least / len(pieces), largest / len(pieces))
        gain = gain * jnp.repeat(jnp.exp(draws), dims[axis_at] // parts).reshape((-1,) + (1,) * (len(dims) - 1 - axis_at))
    return gain


def normal_values(stream_key, shape, width, limit, shards=(), kind=jnp.bfloat16):
    values = width * jax.random.normal(stream_key, shape, jnp.float32)
    if shards:
        values = values * levels(stream_key, shape, shards, -0.22, 0.18)
    return jnp.clip(values, -limit, limit).astype(kind)


def setup_inputs(seed: int = 0) -> dict:
    streams_of = jax.random.split(jax.random.key(seed), 8)
    return {
        "grad": draw_grad(jax.random.fold_in(streams_of[7], 71), 0),
        "param": normal_values(streams_of[1], (N_SHARD * CAP, BLOCK, D), 0.02, 0.119628906, ((0, 8), (1, 4))),
        "row_state": draw_row_state(jax.random.fold_in(streams_of[7], 71), 0),
        "col_state": draw_col_state(jax.random.fold_in(streams_of[7], 71), 0),
        "block_start": draw_block_start(jax.random.fold_in(streams_of[7], 71), 0),
        "block_matrix": draw_block_matrix(jax.random.fold_in(streams_of[7], 71), 0),
        "step": jax.random.randint(streams_of[6], (1,), 2, 12).astype(jnp.int32),
    }


def scale_grad(grad, safe_rows, matrix_pick, new_cols, row_avg):
    slot_cols = jnp.dot(matrix_pick, new_cols, precision=lax.Precision.HIGHEST)
    slot_avg = jnp.dot(matrix_pick, row_avg, precision=lax.Precision.HIGHEST)
    return grad / jnp.sqrt(safe_rows[:, :, None] * slot_cols[:, None, :] / slot_avg[:, None, None])

def reference(grad, param, row_state, col_state, block_start, block_matrix, step):
    slot_total = grad.shape[0]
    block_ends = jnp.concatenate([block_start[1:], jnp.full((1,), NB, jnp.int32)])
    slot_ids = jnp.arange(slot_total, dtype=jnp.int32)
    owner_shard = slot_ids // CAP
    within = slot_ids % CAP
    owned_count = (block_ends - block_start)[owner_shard]
    live_slot = within < owned_count
    block_ids = jnp.minimum(block_start[owner_shard] + within, NB - 1).astype(jnp.int32)
    matrix_ids = jnp.where(live_slot, block_matrix[block_ids], 0)
    matrix_pick = (matrix_ids[:, None] == jnp.arange(3, dtype=jnp.int32)[None, :]).astype(jnp.float32)
    member = matrix_pick * live_slot[:, None].astype(jnp.float32)
    row_count = jnp.array([D, D, FF], jnp.float32)
    step_value = step[0].astype(jnp.float32)
    decay_rate = 1.0 - step_value ** (-0.8)
    learn_rate = 1.0 / jnp.sqrt(jnp.maximum(step_value, 10000.0))
    squares = grad * grad
    new_rows = jnp.where(live_slot[:, None], decay_rate * row_state + (1.0 - decay_rate) * lax.optimization_barrier(jnp.sum(squares, axis=2)) / D, 0.0)
    safe_rows = jnp.where(live_slot[:, None], new_rows, 1.0)
    col_total = jnp.einsum('sm,sd->md', member, lax.optimization_barrier(jnp.sum(squares, axis=1)), precision=lax.Precision.HIGHEST)
    new_cols = decay_rate * col_state + (1.0 - decay_rate) * col_total / row_count[:, None]
    row_avg = jnp.dot(lax.optimization_barrier(jnp.sum(new_rows, axis=1)), member, precision=lax.Precision.HIGHEST) / row_count
    scaled = scale_grad(grad, safe_rows, matrix_pick, new_cols, row_avg)
    square_total = jnp.dot(lax.optimization_barrier(jnp.sum(scaled * scaled, axis=(1, 2))), member, precision=lax.Precision.HIGHEST)
    clip_factor = jnp.maximum(1.0, jnp.sqrt(square_total / (row_count * D)))
    slot_clip = jnp.dot(matrix_pick, clip_factor, precision=lax.Precision.HIGHEST)
    updated = jnp.where(live_slot[:, None, None], param.astype(jnp.float32) - learn_rate * scaled / slot_clip[:, None, None], 0.0).astype(jnp.bfloat16)
    block_index = jnp.arange(NB, dtype=jnp.int32)
    block_owner = lax.optimization_barrier(jnp.sum((block_start[None, :] <= block_index[:, None]).astype(jnp.int32), axis=1)) - 1
    slot_of = (block_owner * CAP + block_index - jnp.take(block_start, block_owner)).astype(jnp.int32)
    new_params = jnp.take(updated, slot_of, axis=0).reshape(NB * BLOCK, D)
    return (new_params, new_rows, new_cols)
```

```python
import functools

import jax
import jax.numpy as jnp
from jax import lax
from jax.experimental import pallas as pl
from jax.experimental.pallas import tpu as pltpu
from jax.sharding import PartitionSpec as P

D = 4096
FF = 10240
MATS = 3
CHUNK = 8


def slots_per_step(slot_count):
    return max(n for n in range(1, 5) if slot_count % n == 0)


def sums_kernel(group, mats, piece, ints_ref, floats_ref, grad_ref, state_ref, rows_ref, sums_ref, cols_acc, weighted_acc, rows_acc):
    step = pl.program_id(0)
    owned = ints_ref[0]
    beta = floats_ref[0]
    gain = floats_ref[1]
    height, width = grad_ref.shape[1], grad_ref.shape[2]

    @pl.when(step == 0)
    def _():
        cols_acc[...] = jnp.zeros_like(cols_acc)
        weighted_acc[...] = jnp.zeros_like(weighted_acc)
        rows_acc[...] = jnp.zeros_like(rows_acc)

    for j in range(group):
        slot = step * group + j

        @pl.when(slot >= owned)
        def _():
            rows_ref[j] = jnp.zeros_like(rows_ref[j])

        @pl.when(slot < owned)
        def _():
            m = ints_ref[2 + slot]
            squares = grad_ref[j] * grad_ref[j]
            rows = beta * state_ref[j] + gain * jnp.sum(squares, axis=1, keepdims=True)
            rows_ref[j] = rows
            tall = (height // 8, 8, width)
            cols_acc[m] += jnp.sum(squares.reshape(tall), axis=0)
            weighted_acc[m] += jnp.sum((squares * (1.0 / rows)).reshape(tall), axis=0)
            rows_acc[m] += jnp.sum(jnp.broadcast_to(rows, (height, 128)).reshape(height // 8, 8, 128), axis=0)

    @pl.when(step == pl.num_programs(0) - 1)
    def _():
        sums_ref[...] = jnp.zeros_like(sums_ref)
        for m in range(mats):
            sums_ref[m : m + 1, :] = jnp.sum(cols_acc[m], axis=0, keepdims=True)
            sums_ref[mats + m : mats + m + 1, :] = jnp.sum(weighted_acc[m], axis=0, keepdims=True)
            spot = lax.broadcasted_iota(jnp.int32, (1, sums_ref.shape[1]), 1) % piece == m
            part = jnp.sum(rows_acc[m], axis=0, keepdims=True)[:, 0:1]
            sums_ref[2 * mats : 2 * mats + 1, :] += jnp.where(spot, part, 0.0)


def main_kernel(mats, row_counts, ids_ref, spots_ref, floats_ref, sums_ref, state_ref, rows_ref, grad_ref, param_ref, temp_ref, cols_ref, *scratch):
    (grad_buf, param_buf, send_buf, picked, factor, part_in, part_all, total_all) = scratch[:8]
    (load_sem, part_sem, cross_send, cross_recv, line_send, line_recv, own_sem) = scratch[8:15]
    recv_bufs = scratch[15:]
    parts, copies = lax.axis_size("shard"), lax.axis_size("dp")
    me, z = lax.axis_index("shard"), lax.axis_index("dp")
    row_groups, slot_count, _, width = grad_buf.shape
    units = len(recv_bufs)
    cut = width // parts
    col_groups = units // row_groups
    blocks = picked.shape[1]
    beta, rest, rate = floats_ref[0], floats_ref[2], floats_ref[3]

    def wait(ref, sem):
        pltpu.make_async_copy(ref, ref, sem).wait()

    def loads(k):
        rows = pl.ds(k * CHUNK, CHUNK)
        return (
            pltpu.make_async_copy(grad_ref.at[:, rows, :], grad_buf.at[k], load_sem.at[0, k]),
            pltpu.make_async_copy(param_ref.at[:, rows, :], param_buf.at[k], load_sem.at[1, k]),
        )

    def send(src, dst, send_sem, recv_sem, axis, to):
        pltpu.make_async_remote_copy(
            src_ref=src,
            dst_ref=dst,
            send_sem=send_sem,
            recv_sem=recv_sem,
            device_id={axis: to},
            device_id_type=pl.DeviceIdType.MESH,
        ).start()

    for copy in loads(0):
        copy.start()

    barrier = pltpu.get_barrier_semaphore()
    for axis, at, size in (("shard", me, parts), ("dp", z, copies)):
        for step in range(1, size):
            peer = lax.rem(at + step, size)
            pl.semaphore_signal(barrier, inc=1, device_id={axis: peer}, device_id_type=pl.DeviceIdType.MESH)
    pl.semaphore_wait(barrier, parts + copies - 2)

    for step in range(1, parts):
        to = lax.rem(me + step, parts)
        span = pl.ds(pl.multiple_of(to * cut, 128), cut)
        send(sums_ref.at[:, span], part_in.at[me], part_sem.at[0], part_sem.at[1], "shard", to)
    mine = pl.ds(pl.multiple_of(me * cut, 128), cut)
    pltpu.make_async_copy(sums_ref.at[:, mine], part_in.at[me], part_sem.at[1]).start()
    wait(part_in, part_sem.at[1])
    part_all[z] = jnp.sum(part_in[...], axis=0)
    for step in range(1, copies):
        to = lax.rem(z + step, copies)
        send(part_all.at[z], part_all.at[z], part_sem.at[2], part_sem.at[3], "dp", to)
    wait(part_all.at[pl.ds(0, copies - 1)], part_sem.at[3])
    total_all[me] = jnp.sum(part_all[...], axis=0)
    for step in range(1, parts):
        to = lax.rem(me + step, parts)
        send(total_all.at[me], total_all.at[me], part_sem.at[4], part_sem.at[5], "shard", to)
    for k in range(1, row_groups):
        for copy in loads(k):
            copy.start()
    wait(total_all.at[pl.ds(0, parts - 1)], part_sem.at[5])

    for m in range(mats):
        count = row_counts[m]
        square = jnp.zeros((1, 1), jnp.float32)
        for s in range(parts):
            span = slice(s * cut, (s + 1) * cut)
            cols = beta * state_ref[m : m + 1, span] + rest * (total_all[s, m : m + 1, :] / count)
            cols_ref[m : m + 1, span] = cols
            square += jnp.sum(total_all[s, mats + m : mats + m + 1, :] / cols, axis=1, keepdims=True)
        average = total_all[0, 2 * mats : 2 * mats + 1, m : m + 1] / count
        clip = jnp.maximum(1.0, jnp.sqrt(average * square / (count * width)))
        gain = jnp.sqrt(average) * rate / clip
        for s in range(parts):
            span = slice(s * cut, (s + 1) * cut)
            factor[m, :, span] = jnp.broadcast_to(lax.rsqrt(cols_ref[m : m + 1, span]) * gain, (CHUNK, cut))

    def update(k):
        for copy in loads(k):
            copy.wait()
        for c in range(col_groups):
            u = k * col_groups + c

            def slot(j, carry):
                m = ids_ref[j]
                scale = lax.rsqrt(rows_ref[j, k * CHUNK : (k + 1) * CHUNK, :])
                for s in range(parts):
                    span = slice(s * cut + c * 128, s * cut + (c + 1) * 128)
                    new = param_buf[k, j, :, span].astype(jnp.float32) - grad_buf[k, j, :, span] * scale * factor[m, :, span]
                    send_buf[u, s, j] = new.astype(send_buf.dtype)
                return carry

            lax.fori_loop(0, slot_count, slot, 0)
            spot = pl.ds(me * slot_count, slot_count)
            for step in range(1, parts):
                to = lax.rem(me + step, parts)
                send(send_buf.at[u, to], recv_bufs[u].at[spot], cross_send.at[u], cross_recv.at[u], "shard", to)
            pltpu.make_async_copy(send_buf.at[u, me], recv_bufs[u].at[spot], cross_recv.at[u]).start()

    def own(u):
        wait(recv_bufs[u], cross_recv.at[u])

        def pick(b, carry):
            picked[u, b] = recv_bufs[u][spots_ref[b]]
            return carry

        lax.fori_loop(0, blocks, pick, 0, unroll=8)

        @pl.when(z < copies - 1)
        def _():
            send(picked.at[u], temp_ref.at[z, u], line_send.at[0, 0], line_recv.at[0, 0, u], "dp", z + 1)

        @pl.when(z > 0)
        def _():
            send(picked.at[u], temp_ref.at[z, u], line_send.at[1, 0], line_recv.at[1, 0, u], "dp", z - 1)

        pltpu.make_async_copy(picked.at[u], temp_ref.at[z, u], own_sem).start()

    def forward(h, u):
        @pl.when((z >= h) & (z < copies - 1))
        def _():
            block = temp_ref.at[z - h, u]
            wait(block, line_recv.at[0, h - 1, u])
            send(block, block, line_send.at[0, h], line_recv.at[0, h, u], "dp", z + 1)

        @pl.when((z + h < copies) & (z > 0))
        def _():
            block = temp_ref.at[z + h, u]
            wait(block, line_recv.at[1, h - 1, u])
            send(block, block, line_send.at[1, h], line_recv.at[1, h, u], "dp", z - 1)

    early = min(row_groups, 2)
    for k in range(early):
        update(k)
    later = list(range(early, row_groups))
    for i in range(units + copies - 2):
        if i < units:
            own(i)
        if later:
            update(later.pop(0))
        for h in range(1, copies - 1):
            if 0 <= i - h < units:
                forward(h, i - h)

    for h in range(1, copies):
        for u in range(units):
            @pl.when((z >= h) & (z == copies - 1))
            def _():
                wait(temp_ref.at[z - h, u], line_recv.at[0, h - 1, u])

            @pl.when((z + h < copies) & (z == 0))
            def _():
                wait(temp_ref.at[z + h, u], line_recv.at[1, h - 1, u])

    for h in range(copies - 1):
        @pl.when((z >= h) & (z < copies - 1))
        def _():
            wait(temp_ref.at[0], line_send.at[0, h])

        @pl.when((z + h < copies) & (z > 0))
        def _():
            wait(temp_ref.at[0], line_send.at[1, h])

    wait(temp_ref.at[0], own_sem)
    for u in range(units):
        wait(send_buf.at[u, pl.ds(0, parts - 1)], cross_send.at[u])
    wait(part_in.at[pl.ds(0, parts - 1)], part_sem.at[0])
    wait(part_all.at[pl.ds(0, copies - 1)], part_sem.at[2])
    wait(total_all.at[pl.ds(0, parts - 1)], part_sem.at[4])


def place_kernel(in_ref, out_ref):
    copies, row_groups = out_ref.shape[1], out_ref.shape[2]
    col_groups = in_ref.shape[1] // row_groups
    for d in range(copies):
        for k in range(row_groups):
            for c in range(col_groups):
                out_ref[:, d, k, :, c * 128 : (c + 1) * 128] = in_ref[d, k * col_groups + c]


def body(parts, grad, param, row_state, col_state, block_start, block_matrix, step):
    slot_count, height, width = grad.shape
    mats = col_state.shape[0]
    total_blocks = block_matrix.shape[0]
    group = slots_per_step(slot_count)
    steps = slot_count // group
    chunks = height // CHUNK
    cut = width // parts
    row_counts = (float(D), float(D), float(FF))

    shard_index = lax.axis_index("shard")
    block_ends = jnp.concatenate([block_start[1:], jnp.full((1,), total_blocks, jnp.int32)])
    at_shard = jnp.arange(parts, dtype=jnp.int32) == shard_index
    first_block = jnp.sum(jnp.where(at_shard, block_start, 0))
    owned = jnp.sum(jnp.where(at_shard, block_ends - block_start, 0))
    block_index = jnp.arange(total_blocks, dtype=jnp.int32)
    slot_blocks = first_block + jnp.arange(slot_count, dtype=jnp.int32)
    matrix_ids = jnp.sum(
        jnp.where(slot_blocks[:, None] == block_index[None, :], block_matrix[None, :], 0), axis=1
    )
    started = block_start[None, :] <= block_index[:, None]
    owner = jnp.sum(started.astype(jnp.int32), axis=1) - 1
    owner_start = jnp.max(jnp.where(started, block_start[None, :], 0), axis=1)
    slot_of = owner * slot_count + block_index - owner_start
    ints = jnp.concatenate([jnp.stack([owned, (owned - 1) // group]), matrix_ids]).astype(jnp.int32)
    step_value = step[0].astype(jnp.float32)
    beta = 1.0 - step_value ** (-0.8)
    rate = 1.0 / jnp.sqrt(jnp.maximum(step_value, 10000.0))
    floats = jnp.stack([beta, (1.0 - beta) / width, 1.0 - beta, rate])

    smem = pl.BlockSpec(memory_space=pltpu.SMEM)

    def live(i, ints_ref):
        return jnp.minimum(i, ints_ref[1])

    new_rows, sums = pl.pallas_call(
        functools.partial(sums_kernel, group, mats, cut),
        grid_spec=pltpu.PrefetchScalarGridSpec(
            num_scalar_prefetch=1,
            grid=(steps,),
            in_specs=[
                smem,
                pl.BlockSpec((group, height, width), lambda i, s: (live(i, s), 0, 0)),
                pl.BlockSpec((group, height, 1), lambda i, s: (i, 0, 0)),
            ],
            out_specs=[
                pl.BlockSpec((group, height, 1), lambda i, s: (i, 0, 0)),
                pl.BlockSpec((8, width), lambda i, s: (0, 0)),
            ],
            scratch_shapes=[
                pltpu.VMEM((mats, 8, width), jnp.float32),
                pltpu.VMEM((mats, 8, width), jnp.float32),
                pltpu.VMEM((mats, 8, 128), jnp.float32),
            ],
        ),
        out_shape=[
            jax.ShapeDtypeStruct((slot_count, height, 1), jnp.float32),
            jax.ShapeDtypeStruct((8, width), jnp.float32),
        ],
        compiler_params=pltpu.CompilerParams(vmem_limit_bytes=60 * 2**20),
        cost_estimate=pl.CostEstimate(flops=grad.size * 6, bytes_accessed=grad.size * 4, transcendentals=0),
        name="sums",
    )(ints, floats, grad, row_state[:, :, None])

    copies = lax.axis_size("dp")
    units = chunks * (cut // 128)
    vmem = pl.BlockSpec(memory_space=pltpu.VMEM)
    hbm = pl.BlockSpec(memory_space=pl.ANY)
    dma = pltpu.SemaphoreType.DMA
    temp, new_cols = pl.pallas_call(
        functools.partial(main_kernel, mats, row_counts),
        in_specs=[smem, smem, smem, vmem, vmem, vmem, hbm, hbm],
        out_specs=[hbm, vmem],
        out_shape=[
            jax.ShapeDtypeStruct((copies, units, total_blocks, CHUNK, 128), jnp.bfloat16),
            jax.ShapeDtypeStruct((mats, width), jnp.float32),
        ],
        scratch_shapes=[
            pltpu.VMEM((chunks, slot_count, CHUNK, width), jnp.float32),
            pltpu.VMEM((chunks, slot_count, CHUNK, width), jnp.bfloat16),
            pltpu.VMEM((units, parts, slot_count, CHUNK, 128), jnp.bfloat16),
            pltpu.VMEM((units, total_blocks, CHUNK, 128), jnp.bfloat16),
            pltpu.VMEM((mats, CHUNK, width), jnp.float32),
            pltpu.VMEM((parts, 8, cut), jnp.float32),
            pltpu.VMEM((copies, 8, cut), jnp.float32),
            pltpu.VMEM((parts, 8, cut), jnp.float32),
            dma((2, chunks)),
            dma((6,)),
            dma((units,)),
            dma((units,)),
            dma((2, copies - 1)),
            dma((2, copies - 1, units)),
            dma(()),
        ]
        + [pltpu.VMEM((parts * slot_count, CHUNK, 128), jnp.bfloat16) for _ in range(units)],
        compiler_params=pltpu.CompilerParams(
            collective_id=0, has_side_effects=True, vmem_limit_bytes=63 * 2**20
        ),
        cost_estimate=pl.CostEstimate(flops=grad.size * 6, bytes_accessed=grad.size * 8, transcendentals=0),
        name="main",
    )(matrix_ids, slot_of, floats, sums, col_state, new_rows, grad, param)

    run = 12 if total_blocks % 12 == 0 else 1
    placed = pl.pallas_call(
        place_kernel,
        grid=(total_blocks // run,),
        in_specs=[pl.BlockSpec((copies, units, run, CHUNK, 128), lambda i: (0, 0, i, 0, 0))],
        out_specs=pl.BlockSpec((run, copies, chunks, CHUNK, cut), lambda i: (i, 0, 0, 0, 0)),
        out_shape=jax.ShapeDtypeStruct((total_blocks, copies, chunks, CHUNK, cut), jnp.bfloat16),
        compiler_params=pltpu.CompilerParams(vmem_limit_bytes=60 * 2**20),
        cost_estimate=pl.CostEstimate(flops=0, bytes_accessed=2 * total_blocks * copies * height * cut * 2, transcendentals=0),
        name="place",
    )(temp)
    new_params = placed.reshape(total_blocks * copies * height, cut)
    return new_params, new_rows[:, :, 0], new_cols


def solution(mesh):
    return jax.shard_map(
        functools.partial(body, mesh.shape["shard"]),
        mesh=mesh,
        in_specs=(
            P("shard", "dp", None),
            P("shard", "dp", None),
            P("shard", "dp"),
            P(),
            P(),
            P(),
            P(),
        ),
        out_specs=(P(None, "shard"), P("shard", "dp"), P()),
        check_vma=False,
    )
```

```python
import functools

import jax
import jax.numpy as jnp
from jax import lax
from jax.experimental import pallas as pl
from jax.experimental.pallas import tpu as pltpu
from jax.sharding import PartitionSpec as P

D = 4096
FF = 10240
MATS = 3
CHUNK = 8


def largest(limit, count):
    return max(n for n in range(1, limit + 1) if count % n == 0)


def wait(ref, sem):
    pltpu.make_async_copy(ref, ref, sem).wait()


def first_and_owned(start_ref, blocks):
    parts = start_ref.shape[0]
    me = lax.axis_index("shard")
    first = start_ref[me]
    end = jnp.where(me == parts - 1, blocks, start_ref[jnp.minimum(me + 1, parts - 1)])
    return first, end - first


def decay_of(step_ref, shape):
    return jnp.exp(-0.8 * jnp.log(jnp.full(shape, step_ref[0], jnp.int32).astype(jnp.float32)))


def sums_kernel(group, mats, cut, start_ref, matrix_ref, step_ref, grad_ref, state_ref, rows_ref, scale_ref, sums_ref, cols_acc, weighted_acc, rows_acc):
    i = pl.program_id(0)
    blocks = matrix_ref.shape[0]
    first, owned = first_and_owned(start_ref, blocks)
    height, width = grad_ref.shape[1], grad_ref.shape[2]
    spans = [slice(n, n + 128) for n in range(0, width, 128)]

    def fold(tile):
        parts = [tile[n : n + 8] for n in range(0, height, 8)]
        while len(parts) > 1:
            parts = [a + b for a, b in zip(parts[::2], parts[1::2])] + parts[len(parts) & ~1 :]
        return parts[0]

    @pl.when(i == 0)
    def _():
        rows_ref[...] = jnp.zeros_like(rows_ref)
        cols_acc[...] = jnp.zeros_like(cols_acc)
        weighted_acc[...] = jnp.zeros_like(weighted_acc)
        rows_acc[...] = jnp.zeros_like(rows_acc)

    @pl.when(i * group < owned)
    def _():
        decay = decay_of(step_ref, (height, 1))
        eye = lax.broadcasted_iota(jnp.int32, (height, height), 0) == lax.broadcasted_iota(jnp.int32, (height, height), 1)
        work = []
        for j in range(group):
            slot = i * group + j
            live = slot < owned
            m = jnp.where(live, matrix_ref[jnp.minimum(first + slot, blocks - 1)], mats)
            across = jnp.zeros((height, 128), jnp.float32)
            for span in spans:
                tile = grad_ref[j, :, span]
                tile = tile * tile
                across += tile
                cols_acc[m, :, span] += fold(tile)
            state = jnp.sum(jnp.where(eye, state_ref[pl.ds(slot, 1), :], 0.0), axis=1, keepdims=True)
            total = jnp.sum(across, axis=1, keepdims=True)
            rows = (1.0 - decay) * state + decay * (total / width)
            flat = jnp.sum(jnp.where(eye, rows, 0.0), axis=0, keepdims=True)
            rows_ref[pl.ds(slot, 1), :] = jnp.where(live, flat, 0.0)
            rows = jnp.broadcast_to(rows, (height, 128))
            scale_ref[j] = lax.rsqrt(rows)
            rows_acc[m] += fold(rows)
            work.append((j, m, 1.0 / rows))
        for j, m, inverse in work:
            for span in spans:
                tile = grad_ref[j, :, span]
                weighted_acc[m, :, span] += fold(tile * tile * inverse)

    @pl.when(i == pl.num_programs(0) - 1)
    def _():
        sums_ref[...] = jnp.zeros_like(sums_ref)
        for m in range(mats):
            sums_ref[m : m + 1, :] = jnp.sum(cols_acc[m], axis=0, keepdims=True)
            sums_ref[mats + m : mats + m + 1, :] = jnp.sum(weighted_acc[m], axis=0, keepdims=True)
            spot = lax.broadcasted_iota(jnp.int32, (1, width), 1) % cut == m
            part = jnp.sum(rows_acc[m], axis=0, keepdims=True)[:, 0:1]
            sums_ref[2 * mats : 2 * mats + 1, :] += jnp.where(spot, part, 0.0)


def main_kernel(mats, row_counts, start_ref, matrix_ref, step_ref, sums_ref, state_ref, scale_ref, grad_ref, param_ref, temp_ref, cols_ref, *scratch):
    (ids, spots, grad_buf, param_buf, scale_buf, send_buf, picked, factor, part_in, part_all, total_all) = scratch[:11]
    (load_sem, part_sem, cross_send, cross_recv, line_send, line_recv, own_sem) = scratch[11:18]
    recv_bufs = scratch[18:]
    parts, copies = lax.axis_size("shard"), lax.axis_size("dp")
    me, z = lax.axis_index("shard"), lax.axis_index("dp")
    row_groups, slot_count, _, width = grad_buf.shape
    units = len(recv_bufs)
    cut = width // parts
    col_groups = units // row_groups
    blocks = picked.shape[1]
    def loads(k):
        rows = pl.ds(k * CHUNK, CHUNK)
        return (
            pltpu.make_async_copy(grad_ref.at[:, rows, :], grad_buf.at[k], load_sem.at[0, k]),
            pltpu.make_async_copy(param_ref.at[:, rows, :], param_buf.at[k], load_sem.at[1, k]),
            pltpu.make_async_copy(scale_ref.at[:, rows, :], scale_buf.at[k], load_sem.at[2, k]),
        )

    def send(src, dst, send_sem, recv_sem, axis, to):
        pltpu.make_async_remote_copy(
            src_ref=src,
            dst_ref=dst,
            send_sem=send_sem,
            recv_sem=recv_sem,
            device_id={axis: to},
            device_id_type=pl.DeviceIdType.MESH,
        ).start()

    for copy in loads(0):
        copy.start()

    barrier = pltpu.get_barrier_semaphore()
    for axis, at, size in (("shard", me, parts), ("dp", z, copies)):
        for step in range(1, size):
            peer = lax.rem(at + step, size)
            pl.semaphore_signal(barrier, inc=1, device_id={axis: peer}, device_id_type=pl.DeviceIdType.MESH)

    first = start_ref[me]

    def note_id(j, carry):
        ids[j] = matrix_ref[jnp.minimum(first + j, blocks - 1)]
        return carry

    def note_spot(b, carry):
        shift = jnp.int32(0)
        for s in range(1, parts):
            shift = jnp.where(b >= start_ref[s], s * slot_count - start_ref[s], shift)
        spots[b] = jnp.minimum(b + shift, parts * slot_count - 1)
        return carry

    lax.fori_loop(0, slot_count, note_id, 0)
    lax.fori_loop(0, blocks, note_spot, 0)
    pl.semaphore_wait(barrier, parts + copies - 2)

    for step in range(1, parts):
        to = lax.rem(me + step, parts)
        span = pl.ds(pl.multiple_of(to * cut, 128), cut)
        send(sums_ref.at[:, span], part_in.at[me], part_sem.at[0], part_sem.at[1], "shard", to)
    mine = pl.ds(pl.multiple_of(me * cut, 128), cut)
    pltpu.make_async_copy(sums_ref.at[:, mine], part_in.at[me], part_sem.at[1]).start()
    wait(part_in, part_sem.at[1])
    part_all[z] = jnp.sum(part_in[...], axis=0)
    for step in range(1, copies):
        to = lax.rem(z + step, copies)
        send(part_all.at[z], part_all.at[z], part_sem.at[2], part_sem.at[3], "dp", to)
    wait(part_all.at[pl.ds(0, copies - 1)], part_sem.at[3])
    total_all[me] = jnp.sum(part_all[...], axis=0)
    for step in range(1, parts):
        to = lax.rem(me + step, parts)
        send(total_all.at[me], total_all.at[me], part_sem.at[4], part_sem.at[5], "shard", to)
    for k in range(1, row_groups):
        for copy in loads(k):
            copy.start()
    wait(total_all.at[pl.ds(0, parts - 1)], part_sem.at[5])

    decay = decay_of(step_ref, (1, 1))
    step = jnp.full((1, 1), step_ref[0], jnp.int32).astype(jnp.float32)
    rate = 1.0 / jnp.sqrt(jnp.maximum(step, 10000.0))
    for m in range(mats):
        count = row_counts[m]
        square = jnp.zeros((1, 1), jnp.float32)
        for s in range(parts):
            span = slice(s * cut, (s + 1) * cut)
            cols = (1.0 - decay) * state_ref[m : m + 1, span] + decay * (total_all[s, m : m + 1, :] / count)
            cols_ref[m : m + 1, span] = cols
            square += jnp.sum(total_all[s, mats + m : mats + m + 1, :] / cols, axis=1, keepdims=True)
        average = total_all[0, 2 * mats : 2 * mats + 1, m : m + 1] / count
        clip = jnp.maximum(1.0, jnp.sqrt(average * square / (count * width)))
        gain = jnp.sqrt(average) * rate / clip
        for s in range(parts):
            span = slice(s * cut, (s + 1) * cut)
            factor[m, :, span] = jnp.broadcast_to(lax.rsqrt(cols_ref[m : m + 1, span]) * gain, (CHUNK, cut))

    unroll = largest(4, slot_count)

    def update(u):
        k, c = u // col_groups, u % col_groups
        if c == 0:
            for copy in loads(k):
                copy.wait()

        def slot(j, carry):
            m = ids[j]
            scale = scale_buf[k, j]
            for s in range(parts):
                span = slice(s * cut + c * 128, s * cut + (c + 1) * 128)
                new = param_buf[k, j, :, span].astype(jnp.float32) - grad_buf[k, j, :, span] * scale * factor[m, :, span]
                send_buf[u, s, j] = new.astype(send_buf.dtype)
            return carry

        lax.fori_loop(0, slot_count, slot, 0, unroll=unroll)
        spot = pl.ds(me * slot_count, slot_count)
        for step in range(1, parts):
            to = lax.rem(me + step, parts)
            send(send_buf.at[u, to], recv_bufs[u].at[spot], cross_send.at[u], cross_recv.at[u], "shard", to)
        pltpu.make_async_copy(send_buf.at[u, me], recv_bufs[u].at[spot], cross_recv.at[u]).start()

    def own(u):
        wait(recv_bufs[u], cross_recv.at[u])

        def pick(b, carry):
            picked[u, b] = recv_bufs[u][spots[b]]
            return carry

        lax.fori_loop(0, blocks, pick, 0, unroll=8)

        @pl.when(z < copies - 1)
        def _():
            send(picked.at[u], temp_ref.at[z, u], line_send.at[0, 0], line_recv.at[0, 0, u], "dp", z + 1)

        @pl.when(z > 0)
        def _():
            send(picked.at[u], temp_ref.at[z, u], line_send.at[1, 0], line_recv.at[1, 0, u], "dp", z - 1)

        pltpu.make_async_copy(picked.at[u], temp_ref.at[z, u], own_sem).start()

    def forward(h, u):
        @pl.when((z >= h) & (z < copies - 1))
        def _():
            block = temp_ref.at[z - h, u]
            wait(block, line_recv.at[0, h - 1, u])
            send(block, block, line_send.at[0, h], line_recv.at[0, h, u], "dp", z + 1)

        @pl.when((z + h < copies) & (z > 0))
        def _():
            block = temp_ref.at[z + h, u]
            wait(block, line_recv.at[1, h - 1, u])
            send(block, block, line_send.at[1, h], line_recv.at[1, h, u], "dp", z - 1)

    early = min(units, 8)
    for u in range(early):
        update(u)
    later = list(range(early, units))
    for i in range(units + copies - 2):
        if i < units:
            own(i)
        for u in later[:4]:
            update(u)
        later = later[4:]
        for h in range(1, copies - 1):
            if 0 <= i - h < units:
                forward(h, i - h)

    for h in range(1, copies):
        for u in range(units):
            @pl.when((z >= h) & (z == copies - 1))
            def _():
                wait(temp_ref.at[z - h, u], line_recv.at[0, h - 1, u])

            @pl.when((z + h < copies) & (z == 0))
            def _():
                wait(temp_ref.at[z + h, u], line_recv.at[1, h - 1, u])

    for h in range(copies - 1):
        @pl.when((z >= h) & (z < copies - 1))
        def _():
            wait(temp_ref.at[0], line_send.at[0, h])

        @pl.when((z + h < copies) & (z > 0))
        def _():
            wait(temp_ref.at[0], line_send.at[1, h])

    wait(temp_ref.at[0], own_sem)
    for u in range(units):
        wait(send_buf.at[u, pl.ds(0, parts - 1)], cross_send.at[u])
    wait(part_in.at[pl.ds(0, parts - 1)], part_sem.at[0])
    wait(part_all.at[pl.ds(0, copies - 1)], part_sem.at[2])
    wait(total_all.at[pl.ds(0, parts - 1)], part_sem.at[4])


def place_kernel(in_ref, out_ref, buf, load_sem, store_sem):
    copies, row_groups = buf.shape[0], buf.shape[1]
    col_groups = in_ref.shape[1] // row_groups
    where = [(d, k) for d in range(copies) for k in range(row_groups)]
    for d, k in where:
        for c in range(col_groups):
            span = slice(c * 128, (c + 1) * 128)
            pltpu.make_async_copy(in_ref.at[d, k * col_groups + c], buf.at[d, k, :, :, span], load_sem.at[d, k]).start()
    for d, k in where:
        wait(buf.at[d, k], load_sem.at[d, k])
        pltpu.make_async_copy(buf.at[d, k], out_ref.at[:, d, k], store_sem).start()
    wait(buf, store_sem)


def body(parts, grad, param, row_state, col_state, block_start, block_matrix, step):
    slot_count, height, width = grad.shape
    mats = col_state.shape[0]
    total_blocks = block_matrix.shape[0]
    group = largest(4, slot_count)
    steps = slot_count // group
    chunks = height // CHUNK
    cut = width // parts
    copies = lax.axis_size("dp")
    units = chunks * (cut // 128)
    row_counts = (float(D), float(D), float(FF))

    smem = pl.BlockSpec(memory_space=pltpu.SMEM)
    vmem = pl.BlockSpec(memory_space=pltpu.VMEM)
    hbm = pl.BlockSpec(memory_space=pl.ANY)
    dma = pltpu.SemaphoreType.DMA

    def live(i, start_ref):
        owned = first_and_owned(start_ref, total_blocks)[1]
        return jnp.minimum(i, (owned - 1) // group)

    new_rows, scale, sums = pl.pallas_call(
        functools.partial(sums_kernel, group, mats, cut),
        grid_spec=pltpu.PrefetchScalarGridSpec(
            num_scalar_prefetch=3,
            grid=(steps,),
            in_specs=[
                pl.BlockSpec((group, height, width), lambda i, s, b, t: (live(i, s), 0, 0)),
                pl.BlockSpec((slot_count, height), lambda i, s, b, t: (0, 0)),
            ],
            out_specs=[
                pl.BlockSpec((slot_count, height), lambda i, s, b, t: (0, 0)),
                pl.BlockSpec((group, height, 128), lambda i, s, b, t: (live(i, s), 0, 0)),
                pl.BlockSpec((8, width), lambda i, s, b, t: (0, 0)),
            ],
            scratch_shapes=[
                pltpu.VMEM((mats + 1, 8, width), jnp.float32),
                pltpu.VMEM((mats + 1, 8, width), jnp.float32),
                pltpu.VMEM((mats + 1, 8, 128), jnp.float32),
            ],
        ),
        out_shape=[
            jax.ShapeDtypeStruct((slot_count, height), jnp.float32),
            jax.ShapeDtypeStruct((slot_count, height, 128), jnp.float32),
            jax.ShapeDtypeStruct((8, width), jnp.float32),
        ],
        compiler_params=pltpu.CompilerParams(vmem_limit_bytes=60 * 2**20),
        cost_estimate=pl.CostEstimate(flops=grad.size * 6, bytes_accessed=grad.size * 4, transcendentals=0),
        name="sums",
    )(block_start, block_matrix, step, grad, row_state)

    temp, new_cols = pl.pallas_call(
        functools.partial(main_kernel, mats, row_counts),
        in_specs=[smem, smem, smem, vmem, vmem, hbm, hbm, hbm],
        out_specs=[hbm, vmem],
        out_shape=[
            jax.ShapeDtypeStruct((copies, units, total_blocks, CHUNK, 128), jnp.bfloat16),
            jax.ShapeDtypeStruct((mats, width), jnp.float32),
        ],
        scratch_shapes=[
            pltpu.SMEM((slot_count,), jnp.int32),
            pltpu.SMEM((total_blocks,), jnp.int32),
            pltpu.VMEM((chunks, slot_count, CHUNK, width), jnp.float32),
            pltpu.VMEM((chunks, slot_count, CHUNK, width), jnp.bfloat16),
            pltpu.VMEM((chunks, slot_count, CHUNK, 128), jnp.float32),
            pltpu.VMEM((units, parts, slot_count, CHUNK, 128), jnp.bfloat16),
            pltpu.VMEM((units, total_blocks, CHUNK, 128), jnp.bfloat16),
            pltpu.VMEM((mats, CHUNK, width), jnp.float32),
            pltpu.VMEM((parts, 8, cut), jnp.float32),
            pltpu.VMEM((copies, 8, cut), jnp.float32),
            pltpu.VMEM((parts, 8, cut), jnp.float32),
            dma((3, chunks)),
            dma((6,)),
            dma((units,)),
            dma((units,)),
            dma((2, copies - 1)),
            dma((2, copies - 1, units)),
            dma(()),
        ]
        + [pltpu.VMEM((parts * slot_count, CHUNK, 128), jnp.bfloat16) for _ in range(units)],
        compiler_params=pltpu.CompilerParams(
            collective_id=0, has_side_effects=True, vmem_limit_bytes=63 * 2**20
        ),
        cost_estimate=pl.CostEstimate(flops=grad.size * 6, bytes_accessed=grad.size * 8, transcendentals=0),
        name="main",
    )(block_start, block_matrix, step, sums, col_state, scale, grad, param)

    placed = pl.pallas_call(
        place_kernel,
        in_specs=[hbm],
        out_specs=hbm,
        out_shape=jax.ShapeDtypeStruct((total_blocks, copies, chunks, CHUNK, cut), jnp.bfloat16),
        scratch_shapes=[
            pltpu.VMEM((copies, chunks, total_blocks, CHUNK, cut), jnp.bfloat16),
            dma((copies, chunks)),
            dma(()),
        ],
        compiler_params=pltpu.CompilerParams(vmem_limit_bytes=60 * 2**20),
        cost_estimate=pl.CostEstimate(flops=0, bytes_accessed=2 * total_blocks * copies * height * cut * 2, transcendentals=0),
        name="place",
    )(temp)
    new_params = placed.reshape(total_blocks * copies * height, cut)
    return new_params, new_rows, new_cols


def solution(mesh):
    return jax.shard_map(
        functools.partial(body, mesh.shape["shard"]),
        mesh=mesh,
        in_specs=(
            P("shard", "dp", None),
            P("shard", "dp", None),
            P("shard", "dp"),
            P(),
            P(),
            P(),
            P(),
        ),
        out_specs=(P(None, "shard"), P("shard", "dp"), P()),
        check_vma=False,
    )
```

```python
import functools

import jax
import jax.numpy as jnp
from jax import lax
from jax.experimental import pallas as pl
from jax.experimental.pallas import tpu as pltpu
from jax.sharding import PartitionSpec as P

D = 4096
FF = 10240
MATS = 3
CHUNK = 8


def largest(limit, count):
    return max(n for n in range(1, limit + 1) if count % n == 0)


def wait(ref, sem):
    pltpu.make_async_copy(ref, ref, sem).wait()


def first_and_owned(start_ref, blocks):
    parts = start_ref.shape[0]
    me = lax.axis_index("shard")
    first = start_ref[me]
    end = jnp.where(me == parts - 1, blocks, start_ref[jnp.minimum(me + 1, parts - 1)])
    return first, end - first


def decay_of(step_ref, shape):
    return jnp.exp(-0.8 * jnp.log(jnp.full(shape, step_ref[0], jnp.int32).astype(jnp.float32)))


def sums_kernel(group, mats, cut, start_ref, matrix_ref, step_ref, state_ref, grad_ref, rows_ref, sums_ref, scale_ref, grad_buf, scale_buf, cols_acc, weighted_acc, rows_acc, load_sem, store_sem):
    blocks = matrix_ref.shape[0]
    first, owned = first_and_owned(start_ref, blocks)
    groups = (owned + group - 1) // group
    height, width = grad_ref.shape[1], grad_ref.shape[2]
    spans = [slice(n, n + 128) for n in range(0, width, 128)]

    def load(i):
        slots = pl.ds(i * group, group)
        return pltpu.make_async_copy(grad_ref.at[slots], grad_buf.at[slots], load_sem.at[i])

    def store(i):
        slots = pl.ds(i * group, group)
        return pltpu.make_async_copy(scale_buf.at[slots], scale_ref.at[slots], store_sem.at[i])

    def start_load(i, carry):
        load(i).start()
        return carry

    lax.fori_loop(0, groups, start_load, 0)

    def fold(tile):
        parts = [tile[n : n + 8] for n in range(0, height, 8)]
        while len(parts) > 1:
            parts = [a + b for a, b in zip(parts[::2], parts[1::2])] + parts[len(parts) & ~1 :]
        return parts[0]

    rows_ref[...] = jnp.zeros_like(rows_ref)
    cols_acc[...] = jnp.zeros_like(cols_acc)
    weighted_acc[...] = jnp.zeros_like(weighted_acc)
    rows_acc[...] = jnp.zeros_like(rows_acc)
    decay = decay_of(step_ref, (height, 1))
    lane = lax.broadcasted_iota(jnp.int32, rows_ref.shape, 1)

    def work(i, carry):
        load(i).wait()
        inverses = []
        for j in range(group):
            slot = i * group + j
            live = slot < owned
            m = jnp.where(live, matrix_ref[jnp.minimum(first + slot, blocks - 1)], mats)
            across = jnp.zeros((height, 128), jnp.float32)
            for span in spans:
                tile = grad_buf[slot, :, span]
                tile = tile * tile
                across += tile
                cols_acc[m, :, span] += fold(tile)
            state = jnp.sum(jnp.where(lane == slot, state_ref[...], 0.0), axis=1, keepdims=True)
            total = jnp.sum(across, axis=1, keepdims=True)
            rows = (1.0 - decay) * state + decay * (total / width)
            rows_ref[...] = jnp.where((lane == slot) & live, rows, rows_ref[...])
            rows = jnp.broadcast_to(rows, (height, 128))
            scale_buf[slot] = lax.rsqrt(rows)
            rows_acc[m] += fold(rows)
            inverses.append((slot, m, 1.0 / rows))
        for slot, m, inverse in inverses:
            for span in spans:
                tile = grad_buf[slot, :, span]
                weighted_acc[m, :, span] += fold(tile * tile * inverse)
        store(i).start()
        return carry

    lax.fori_loop(0, groups, work, 0)
    sums_ref[...] = jnp.zeros_like(sums_ref)
    for m in range(mats):
        sums_ref[m : m + 1, :] = jnp.sum(cols_acc[m], axis=0, keepdims=True)
        sums_ref[mats + m : mats + m + 1, :] = jnp.sum(weighted_acc[m], axis=0, keepdims=True)
        spot = lax.broadcasted_iota(jnp.int32, (1, width), 1) % cut == m
        part = jnp.sum(rows_acc[m], axis=0, keepdims=True)[:, 0:1]
        sums_ref[2 * mats : 2 * mats + 1, :] += jnp.where(spot, part, 0.0)

    def end_store(i, carry):
        store(i).wait()
        return carry

    lax.fori_loop(0, groups, end_store, 0)


def main_kernel(mats, row_counts, start_ref, matrix_ref, step_ref, state_ref, sums_in, scale_ref, grad_ref, param_ref, cols_ref, temp_ref, late_ref, *scratch):
    (ids, spots, sums_ref, grad_buf, param_buf, scale_buf, send_buf, picked, factor, part_in, part_all, total_all) = scratch[:12]
    (load_sem, part_sem, cross_send, cross_recv, line_send, line_recv, own_sem) = scratch[12:19]
    recv_bufs = scratch[19:]
    tail = late_ref.shape[0]
    parts, copies = lax.axis_size("shard"), lax.axis_size("dp")
    me, z = lax.axis_index("shard"), lax.axis_index("dp")
    row_groups, slot_count, _, width = grad_buf.shape
    units = len(recv_bufs)
    cut = width // parts
    col_groups = units // row_groups
    blocks = picked.shape[1]
    def loads(k):
        rows = pl.ds(k * CHUNK, CHUNK)
        return (
            pltpu.make_async_copy(grad_ref.at[:, rows, :], grad_buf.at[k], load_sem.at[0, k]),
            pltpu.make_async_copy(param_ref.at[:, rows, :], param_buf.at[k], load_sem.at[1, k]),
            pltpu.make_async_copy(scale_ref.at[:, rows, :], scale_buf.at[k], load_sem.at[2, k]),
        )

    def send(src, dst, send_sem, recv_sem, axis, to):
        pltpu.make_async_remote_copy(
            src_ref=src,
            dst_ref=dst,
            send_sem=send_sem,
            recv_sem=recv_sem,
            device_id={axis: to},
            device_id_type=pl.DeviceIdType.MESH,
        ).start()

    sums_load = pltpu.make_async_copy(sums_in, sums_ref, part_sem.at[6])
    sums_load.start()
    for copy in loads(0):
        copy.start()

    barrier = pltpu.get_barrier_semaphore()
    for axis, at, size in (("shard", me, parts), ("dp", z, copies)):
        for step in range(1, size):
            peer = lax.rem(at + step, size)
            pl.semaphore_signal(barrier, inc=1, device_id={axis: peer}, device_id_type=pl.DeviceIdType.MESH)

    pl.semaphore_wait(barrier, parts + copies - 2)
    sums_load.wait()

    for step in range(1, parts):
        to = lax.rem(me + step, parts)
        span = pl.ds(pl.multiple_of(to * cut, 128), cut)
        send(sums_ref.at[:, span], part_in.at[me], part_sem.at[0], part_sem.at[1], "shard", to)
    mine = pl.ds(pl.multiple_of(me * cut, 128), cut)
    pltpu.make_async_copy(sums_ref.at[:, mine], part_in.at[me], part_sem.at[1]).start()

    first = start_ref[me]

    def note_id(j, carry):
        ids[j] = matrix_ref[jnp.minimum(first + j, blocks - 1)]
        return carry

    def note_spot(b, carry):
        shift = jnp.int32(0)
        for s in range(1, parts):
            shift = jnp.where(b >= start_ref[s], s * slot_count - start_ref[s], shift)
        spots[b] = jnp.minimum(b + shift, parts * slot_count - 1)
        return carry

    lax.fori_loop(0, slot_count, note_id, 0)
    lax.fori_loop(0, blocks, note_spot, 0)
    wait(part_in, part_sem.at[1])
    part_all[z] = jnp.sum(part_in[...], axis=0)
    for step in range(1, copies):
        to = lax.rem(z + step, copies)
        send(part_all.at[z], part_all.at[z], part_sem.at[2], part_sem.at[3], "dp", to)
    wait(part_all.at[pl.ds(0, copies - 1)], part_sem.at[3])
    total_all[me] = jnp.sum(part_all[...], axis=0)
    for step in range(1, parts):
        to = lax.rem(me + step, parts)
        send(total_all.at[me], total_all.at[me], part_sem.at[4], part_sem.at[5], "shard", to)
    for k in range(1, row_groups):
        for copy in loads(k):
            copy.start()
    wait(total_all.at[pl.ds(0, parts - 1)], part_sem.at[5])

    decay = decay_of(step_ref, (1, 1))
    step = jnp.full((1, 1), step_ref[0], jnp.int32).astype(jnp.float32)
    rate = 1.0 / jnp.sqrt(jnp.maximum(step, 10000.0))
    for m in range(mats):
        count = row_counts[m]
        square = jnp.zeros((1, 1), jnp.float32)
        for s in range(parts):
            span = slice(s * cut, (s + 1) * cut)
            cols = (1.0 - decay) * state_ref[m : m + 1, span] + decay * (total_all[s, m : m + 1, :] / count)
            cols_ref[m : m + 1, span] = cols
            square += jnp.sum(total_all[s, mats + m : mats + m + 1, :] / cols, axis=1, keepdims=True)
        average = total_all[0, 2 * mats : 2 * mats + 1, m : m + 1] / count
        clip = jnp.maximum(1.0, jnp.sqrt(average * square / (count * width)))
        gain = jnp.sqrt(average) * rate / clip
        for s in range(parts):
            span = slice(s * cut, (s + 1) * cut)
            factor[m, :, span] = jnp.broadcast_to(lax.rsqrt(cols_ref[m : m + 1, span]) * gain, (CHUNK, cut))

    unroll = largest(4, slot_count)

    def update(u):
        k, c = u // col_groups, u % col_groups
        if c == 0:
            for copy in loads(k):
                copy.wait()

        def slot(j, carry):
            m = ids[j]
            scale = scale_buf[k, j]
            for s in range(parts):
                span = slice(s * cut + c * 128, s * cut + (c + 1) * 128)
                new = param_buf[k, j, :, span].astype(jnp.float32) - grad_buf[k, j, :, span] * scale * factor[m, :, span]
                send_buf[u, s, j] = new.astype(send_buf.dtype)
            return carry

        lax.fori_loop(0, slot_count, slot, 0, unroll=unroll)
        spot = pl.ds(me * slot_count, slot_count)
        for step in range(1, parts):
            to = lax.rem(me + step, parts)
            send(send_buf.at[u, to], recv_bufs[u].at[spot], cross_send.at[u], cross_recv.at[u], "shard", to)
        pltpu.make_async_copy(send_buf.at[u, me], recv_bufs[u].at[spot], cross_recv.at[u]).start()

    def own(u):
        wait(recv_bufs[u], cross_recv.at[u])

        def pick(b, carry):
            picked[u, b] = recv_bufs[u][spots[b]]
            return carry

        lax.fori_loop(0, blocks, pick, 0, unroll=8)

        @pl.when(z < copies - 1)
        def _():
            send(picked.at[u], temp_ref.at[z, u], line_send.at[0, 0], line_recv.at[0, 0, u], "dp", z + 1)

        @pl.when(z > 0)
        def _():
            send(picked.at[u], temp_ref.at[z, u], line_send.at[1, 0], line_recv.at[1, 0, u], "dp", z - 1)

        pltpu.make_async_copy(picked.at[u], temp_ref.at[z, u], own_sem).start()

    def pass_on(h, u, source, side, to, last):
        block = temp_ref.at[source, u]
        wait(block, line_recv.at[side, h - 1, u])
        if h == copies - 3 and u >= units - tail:
            @pl.when(last)
            def _():
                send(block, late_ref.at[u - units + tail], line_send.at[side, h], line_recv.at[side, h, u], "dp", to)

            @pl.when(jnp.logical_not(last))
            def _():
                send(block, block, line_send.at[side, h], line_recv.at[side, h, u], "dp", to)
        else:
            send(block, block, line_send.at[side, h], line_recv.at[side, h, u], "dp", to)

    def forward(h, u):
        if h == copies - 2 and u >= units - tail:
            return

        @pl.when((z >= h) & (z < copies - 1))
        def _():
            pass_on(h, u, z - h, 0, z + 1, z == copies - 3)

        @pl.when((z + h < copies) & (z > 0))
        def _():
            pass_on(h, u, z + h, 1, z - 1, z == 2)

    early = min(units, 8)
    for u in range(early):
        update(u)
    later = list(range(early, units))
    for i in range(units + copies - 2):
        if i < units:
            own(i)
        for u in later[:4]:
            update(u)
        later = later[4:]
        for h in range(1, copies - 1):
            if 0 <= i - h < units:
                forward(h, i - h)

    for h in range(1, copies):
        for u in range(units - tail if h == copies - 1 else units):
            @pl.when(z == copies - 1)
            def _():
                wait(temp_ref.at[z - h, u], line_recv.at[0, h - 1, u])

            @pl.when(z == 0)
            def _():
                wait(temp_ref.at[z + h, u], line_recv.at[1, h - 1, u])

    for t in range(tail):
        @pl.when(z == copies - 2)
        def _():
            wait(late_ref.at[t], line_recv.at[0, copies - 3, units - tail + t])

        @pl.when(z == 1)
        def _():
            wait(late_ref.at[t], line_recv.at[1, copies - 3, units - tail + t])

    for h in range(copies - 1):
        sent = temp_ref.at[0, pl.ds(0, units - tail if h == copies - 2 else units)]

        @pl.when((z >= h) & (z < copies - 1))
        def _():
            wait(sent, line_send.at[0, h])

        @pl.when((z + h < copies) & (z > 0))
        def _():
            wait(sent, line_send.at[1, h])

    wait(temp_ref.at[0], own_sem)
    for u in range(units):
        wait(send_buf.at[u, pl.ds(0, parts - 1)], cross_send.at[u])
    wait(part_in.at[pl.ds(0, parts - 1)], part_sem.at[0])
    wait(part_all.at[pl.ds(0, copies - 1)], part_sem.at[2])
    wait(total_all.at[pl.ds(0, parts - 1)], part_sem.at[4])


def late_source(copies):
    z = lax.axis_index("dp")
    return jnp.where(z >= copies - 2, 0, jnp.where(z <= 1, copies - 1, copies))


def place_kernel(tail, cols_in, in_ref, late_ref, cols_out, out_ref, buf, group_load, group_store, load_sem, store_sem, late_load, late_store):
    copies, row_groups = buf.shape[0], buf.shape[1]
    units = in_ref.shape[1]
    col_groups = units // row_groups
    skip = late_source(copies)
    z = lax.axis_index("dp")
    inner = (z == 1) | (z == copies - 2)
    cols_out[...] = cols_in[...]
    full = (units - tail) // col_groups
    groups = [(k, d) for k in range(full) for d in range(copies)]
    singles = [(u, d) for u in range(full * col_groups, units) for d in range(copies)]

    def load(u, d, sem):
        k, c = u // col_groups, u % col_groups
        return pltpu.make_async_copy(in_ref.at[d, u], buf.at[d, k, :, :, c * 128 : (c + 1) * 128], sem)

    def store(u, d):
        k, span = u // col_groups, slice(u % col_groups * 128, (u % col_groups + 1) * 128)
        return pltpu.make_async_copy(buf.at[d, k, :, :, span], out_ref.at[:, d, k, :, span], store_sem.at[d, u])

    def group_copy(k, d):
        return pltpu.make_async_copy(buf.at[d, k], out_ref.at[:, d, k], group_store.at[d, k])

    def each(u, d, work):
        if u < units - tail:
            work()
        else:
            pl.when(d != skip)(work)

    for k, d in groups:
        for c in range(col_groups):
            load(k * col_groups + c, d, group_load.at[d, k]).start()
    def load_late(u):
        k, c = u // col_groups, u % col_groups
        return pltpu.make_async_copy(late_ref.at[u - units + tail], buf.at[skip, k, :, :, c * 128 : (c + 1) * 128], late_load.at[u - units + tail])

    def store_late(u):
        k, span = u // col_groups, slice(u % col_groups * 128, (u % col_groups + 1) * 128)
        return pltpu.make_async_copy(buf.at[skip, k, :, :, span], out_ref.at[:, skip, k, :, span], late_store.at[u - units + tail])

    late_units = range(units - tail, units)
    for u, d in singles:
        each(u, d, lambda: load(u, d, load_sem.at[d, u]).start())

    @pl.when(inner)
    def _():
        for u in late_units:
            load_late(u).start()

    for k, d in groups:
        wait(buf.at[d, k], group_load.at[d, k])
        group_copy(k, d).start()
    for u, d in singles:
        def move():
            load(u, d, load_sem.at[d, u]).wait()
            store(u, d).start()

        each(u, d, move)

    @pl.when(inner)
    def _():
        for u in late_units:
            load_late(u).wait()
            store_late(u).start()

    for k, d in groups:
        group_copy(k, d).wait()
    for u, d in singles:
        each(u, d, lambda: store(u, d).wait())

    @pl.when(inner)
    def _():
        for u in late_units:
            store_late(u).wait()


def place_late_kernel(landed_ref, old_ref, out_ref, store_sem):
    tail = landed_ref.shape[0]
    copies, row_groups = out_ref.shape[1], out_ref.shape[2]
    col_groups = out_ref.shape[4] // 128
    z = lax.axis_index("dp")
    skip = late_source(copies)

    def store(t):
        u = row_groups * col_groups - tail + t
        k, span = u // col_groups, slice(u % col_groups * 128, (u % col_groups + 1) * 128)
        return pltpu.make_async_copy(landed_ref.at[t], out_ref.at[:, skip, k, :, span], store_sem.at[t])

    @pl.when((z == 0) | (z == copies - 1))
    def _():
        for t in range(tail):
            store(t).start()
        for t in range(tail):
            store(t).wait()


def body(parts, grad, param, row_state, col_state, block_start, block_matrix, step):
    slot_count, height, width = grad.shape
    mats = col_state.shape[0]
    total_blocks = block_matrix.shape[0]
    group = largest(4, slot_count)
    steps = slot_count // group
    chunks = height // CHUNK
    cut = width // parts
    copies = lax.axis_size("dp")
    assert copies > 3
    units = chunks * (cut // 128)
    tail = min(2, units - 1)
    row_counts = (float(D), float(D), float(FF))

    smem = pl.BlockSpec(memory_space=pltpu.SMEM)
    vmem = pl.BlockSpec(memory_space=pltpu.VMEM)
    hbm = pl.BlockSpec(memory_space=pl.ANY)
    dma = pltpu.SemaphoreType.DMA

    new_rows, sums, scale = pl.pallas_call(
        functools.partial(sums_kernel, group, mats, cut),
        in_specs=[smem, smem, smem, vmem, hbm],
        out_specs=[vmem, vmem, hbm],
        out_shape=[
            jax.ShapeDtypeStruct((height, slot_count), jnp.float32),
            jax.ShapeDtypeStruct((8, width), jnp.float32),
            jax.ShapeDtypeStruct((slot_count, height, 128), jnp.float32),
        ],
        scratch_shapes=[
            pltpu.VMEM((slot_count, height, width), jnp.float32),
            pltpu.VMEM((slot_count, height, 128), jnp.float32),
            pltpu.VMEM((mats + 1, 8, width), jnp.float32),
            pltpu.VMEM((mats + 1, 8, width), jnp.float32),
            pltpu.VMEM((mats + 1, 8, 128), jnp.float32),
            dma((steps,)),
            dma((steps,)),
        ],
        compiler_params=pltpu.CompilerParams(vmem_limit_bytes=60 * 2**20),
        cost_estimate=pl.CostEstimate(flops=grad.size * 6, bytes_accessed=grad.size * 4, transcendentals=0),
        name="sums",
    )(block_start, block_matrix, step, row_state.T, grad)

    new_cols, temp, late = pl.pallas_call(
        functools.partial(main_kernel, mats, row_counts),
        in_specs=[smem, smem, smem, vmem, hbm, hbm, hbm, hbm],
        out_specs=[vmem, hbm, hbm],
        out_shape=[
            jax.ShapeDtypeStruct((mats, width), jnp.float32),
            jax.ShapeDtypeStruct((copies, units, total_blocks, CHUNK, 128), jnp.bfloat16),
            jax.ShapeDtypeStruct((tail, total_blocks, CHUNK, 128), jnp.bfloat16),
        ],
        scratch_shapes=[
            pltpu.SMEM((slot_count,), jnp.int32),
            pltpu.SMEM((total_blocks,), jnp.int32),
            pltpu.VMEM((8, width), jnp.float32),
            pltpu.VMEM((chunks, slot_count, CHUNK, width), jnp.float32),
            pltpu.VMEM((chunks, slot_count, CHUNK, width), jnp.bfloat16),
            pltpu.VMEM((chunks, slot_count, CHUNK, 128), jnp.float32),
            pltpu.VMEM((units, parts, slot_count, CHUNK, 128), jnp.bfloat16),
            pltpu.VMEM((units, total_blocks, CHUNK, 128), jnp.bfloat16),
            pltpu.VMEM((mats, CHUNK, width), jnp.float32),
            pltpu.VMEM((parts, 8, cut), jnp.float32),
            pltpu.VMEM((copies, 8, cut), jnp.float32),
            pltpu.VMEM((parts, 8, cut), jnp.float32),
            dma((3, chunks)),
            dma((7,)),
            dma((units,)),
            dma((units,)),
            dma((2, copies - 1)),
            dma((2, copies - 1, units)),
            dma(()),
        ]
        + [pltpu.VMEM((parts * slot_count, CHUNK, 128), jnp.bfloat16) for _ in range(units)],
        compiler_params=pltpu.CompilerParams(
            collective_id=0, has_side_effects=True, vmem_limit_bytes=63 * 2**20
        ),
        cost_estimate=pl.CostEstimate(flops=grad.size * 6, bytes_accessed=grad.size * 8, transcendentals=0),
        name="main",
    )(block_start, block_matrix, step, col_state, sums, scale, grad, param)

    landed = lax.ppermute(late, "dp", [(copies - 2, copies - 1), (1, 0)])
    size = total_blocks * copies * height * cut
    placed_shape = jax.ShapeDtypeStruct((total_blocks, copies, chunks, CHUNK, cut), jnp.bfloat16)
    new_cols, placed = pl.pallas_call(
        functools.partial(place_kernel, tail),
        in_specs=[vmem, hbm, hbm],
        out_specs=[vmem, hbm],
        out_shape=[jax.ShapeDtypeStruct((mats, width), jnp.float32), placed_shape],
        scratch_shapes=[
            pltpu.VMEM((copies, chunks, total_blocks, CHUNK, cut), jnp.bfloat16),
            dma((copies, chunks)),
            dma((copies, chunks)),
            dma((copies, units)),
            dma((copies, units)),
            dma((tail,)),
            dma((tail,)),
        ],
        compiler_params=pltpu.CompilerParams(vmem_limit_bytes=60 * 2**20),
        cost_estimate=pl.CostEstimate(flops=size * 10, bytes_accessed=4 * size, transcendentals=0),
        name="place",
    )(new_cols, temp, late)
    placed = pl.pallas_call(
        place_late_kernel,
        in_specs=[hbm, hbm],
        out_specs=hbm,
        out_shape=placed_shape,
        input_output_aliases={1: 0},
        scratch_shapes=[
            dma((tail,)),
        ],
        compiler_params=pltpu.CompilerParams(vmem_limit_bytes=4 * 2**20),
        cost_estimate=pl.CostEstimate(flops=size, bytes_accessed=size, transcendentals=0),
        name="place_late",
    )(landed, placed)
    new_params = placed.reshape(total_blocks * copies * height, cut)
    return new_params, new_rows.T, new_cols


def solution(mesh):
    return jax.shard_map(
        functools.partial(body, mesh.shape["shard"]),
        mesh=mesh,
        in_specs=(
            P("shard", "dp", None),
            P("shard", "dp", None),
            P("shard", "dp"),
            P(),
            P(),
            P(),
            P(),
        ),
        out_specs=(P(None, "shard"), P("shard", "dp"), P()),
        check_vma=False,
    )
```

```python
import functools

import jax
import jax.numpy as jnp
from jax import lax
from jax.experimental import pallas as pl
from jax.experimental.pallas import tpu as pltpu
from jax.sharding import PartitionSpec as P

D = 4096
FF = 10240
MATS = 3
CHUNK = 8


def largest(limit, count):
    return max(n for n in range(1, limit + 1) if count % n == 0)


def wait(ref, sem):
    pltpu.make_async_copy(ref, ref, sem).wait()


def first_and_owned(start_ref, blocks):
    parts = start_ref.shape[0]
    me = lax.axis_index("shard")
    first = start_ref[me]
    end = jnp.where(me == parts - 1, blocks, start_ref[jnp.minimum(me + 1, parts - 1)])
    return first, end - first


def decay_of(step_ref, shape):
    return jnp.exp(-0.8 * jnp.log(jnp.full(shape, step_ref[0], jnp.int32).astype(jnp.float32)))


def main_kernel(mats, group, row_counts, start_ref, matrix_ref, step_ref, state_ref, row_state_ref, grad_ref, param_ref, cols_ref, rows_ref, temp_ref, late_ref, *scratch):
    (ids, spots, sums_ref, grad_buf, param_buf, scale_buf, send_buf, picked, factor, part_in, part_all, total_all) = scratch[:12]
    (cols_acc, weighted_acc, rows_acc, grad_sem, param_sem, part_sem, cross_send, cross_recv, line_send, line_recv, own_sem) = scratch[12:23]
    recv_bufs = scratch[23:]
    tail = late_ref.shape[0]
    parts, copies = lax.axis_size("shard"), lax.axis_size("dp")
    me, z = lax.axis_index("shard"), lax.axis_index("dp")
    row_groups, slot_count, _, width = grad_buf.shape
    units = len(recv_bufs)
    cut = width // parts
    col_groups = units // row_groups
    blocks = picked.shape[1]
    def param_load(k):
        rows = pl.ds(k * CHUNK, CHUNK)
        return pltpu.make_async_copy(param_ref.at[:, rows, :], param_buf.at[k], param_sem.at[k])

    def send(src, dst, send_sem, recv_sem, axis, to):
        pltpu.make_async_remote_copy(
            src_ref=src,
            dst_ref=dst,
            send_sem=send_sem,
            recv_sem=recv_sem,
            device_id={axis: to},
            device_id_type=pl.DeviceIdType.MESH,
        ).start()

    for i in range(slot_count // group):
        slots = pl.ds(i * group, group)
        for k in range(row_groups):
            rows = pl.ds(k * CHUNK, CHUNK)
            pltpu.make_async_copy(grad_ref.at[slots, rows, :], grad_buf.at[k, slots], grad_sem.at[i]).start()

    barrier = pltpu.get_barrier_semaphore()
    for axis, at, size in (("shard", me, parts), ("dp", z, copies)):
        for step in range(1, size):
            peer = lax.rem(at + step, size)
            pl.semaphore_signal(barrier, inc=1, device_id={axis: peer}, device_id_type=pl.DeviceIdType.MESH)

    first, owned = first_and_owned(start_ref, blocks)

    def note_id(j, carry):
        ids[j] = jnp.where(j < owned, matrix_ref[jnp.minimum(first + j, blocks - 1)], mats)
        return carry

    lax.fori_loop(0, slot_count, note_id, 0)

    decay = decay_of(step_ref, (1, 1))
    cols_acc[...] = jnp.zeros_like(cols_acc)
    weighted_acc[...] = jnp.zeros_like(weighted_acc)
    rows_acc[...] = jnp.zeros_like(rows_acc)
    rows_ref[...] = jnp.zeros_like(rows_ref)
    lane = lax.broadcasted_iota(jnp.int32, (CHUNK, slot_count), 1)
    spans = [slice(n, n + 128) for n in range(0, width, 128)]

    def add_to(acc, m, span, value):
        for n in range(mats):
            acc[n, :, span] += jnp.where(m == n, value, 0.0)

    def total_of(values):
        while len(values) > 1:
            values = [a + b for a, b in zip(values[::2], values[1::2])] + values[len(values) & ~1 :]
        return values[0]

    def work(i, carry):
        wait(grad_buf.at[:, pl.ds(i * group, group)], grad_sem.at[i])
        inverses = []
        for j in range(group):
            slot = i * group + j
            m = ids[slot]
            across = [jnp.zeros((CHUNK, 128), jnp.float32)] * row_groups
            for span in spans:
                tiles = [grad_buf[k, slot, :, span] for k in range(row_groups)]
                tiles = [tile * tile for tile in tiles]
                across = [a + b for a, b in zip(across, tiles)]
                add_to(cols_acc, m, span, total_of(tiles))
            inverse = []
            for k in range(row_groups):
                at = slice(k * CHUNK, (k + 1) * CHUNK)
                here = lane == slot
                state = jnp.sum(jnp.where(here, row_state_ref[at, :], 0.0), axis=1, keepdims=True)
                rows = (1.0 - decay) * state + decay * (jnp.sum(across[k], axis=1, keepdims=True) / width)
                rows_ref[at, :] = jnp.where(here & (m < mats), rows, rows_ref[at, :])
                rows = jnp.broadcast_to(rows, (CHUNK, 128))
                scale_buf[k, slot] = lax.rsqrt(rows)
                add_to(rows_acc, m, slice(0, 128), rows)
                inverse.append(1.0 / rows)
            inverses.append((slot, m, inverse))
        for slot, m, inverse in inverses:
            for span in spans:
                tiles = [grad_buf[k, slot, :, span] for k in range(row_groups)]
                add_to(weighted_acc, m, span, total_of([tile * tile * inverse[k] for k, tile in enumerate(tiles)]))
        return carry

    lax.fori_loop(0, slot_count // group, work, 0)
    for k in range(row_groups):
        param_load(k).start()
    for m in range(mats):
        sums_ref[m : m + 1, :] = jnp.sum(cols_acc[m], axis=0, keepdims=True)
        sums_ref[mats + m : mats + m + 1, :] = jnp.sum(weighted_acc[m], axis=0, keepdims=True)
    spot = lax.broadcasted_iota(jnp.int32, (1, width), 1) % cut
    rest = jnp.zeros((1, width), jnp.float32)
    for m in range(mats):
        rest = jnp.where(spot == m, jnp.sum(rows_acc[m], axis=0, keepdims=True)[:, 0:1], rest)
    sums_ref[2 * mats :, :] = jnp.broadcast_to(rest, (8 - 2 * mats, width))
    pl.semaphore_wait(barrier, parts + copies - 2)

    for step in range(1, parts):
        to = lax.rem(me + step, parts)
        span = pl.ds(pl.multiple_of(to * cut, 128), cut)
        send(sums_ref.at[:, span], part_in.at[me], part_sem.at[0], part_sem.at[1], "shard", to)
    mine = pl.ds(pl.multiple_of(me * cut, 128), cut)
    pltpu.make_async_copy(sums_ref.at[:, mine], part_in.at[me], part_sem.at[1]).start()

    def note_spot(b, carry):
        shift = jnp.int32(0)
        for s in range(1, parts):
            shift = jnp.where(b >= start_ref[s], s * slot_count - start_ref[s], shift)
        spots[b] = jnp.minimum(b + shift, parts * slot_count - 1)
        return carry

    lax.fori_loop(0, blocks, note_spot, 0)
    wait(part_in, part_sem.at[1])
    part_all[z] = jnp.sum(part_in[...], axis=0)
    for step in range(1, copies):
        to = lax.rem(z + step, copies)
        send(part_all.at[z], part_all.at[z], part_sem.at[2], part_sem.at[3], "dp", to)
    wait(part_all.at[pl.ds(0, copies - 1)], part_sem.at[3])
    total = jnp.sum(part_all[...], axis=0)
    lanes = lax.broadcasted_iota(jnp.int32, (1, cut), 1)
    partial = jnp.zeros((1, cut), jnp.float32)
    for m in range(mats):
        cols = (1.0 - decay) * state_ref[m : m + 1, mine] + decay * (total[m : m + 1] / row_counts[m])
        total_all[me, m : m + 1, :] = cols
        partial = jnp.where(lanes == m, jnp.sum(total[mats + m : mats + m + 1] / cols, axis=1, keepdims=True), partial)
    total_all[me, mats : mats + 1, :] = partial
    for step in range(1, parts):
        to = lax.rem(me + step, parts)
        send(total_all.at[me], total_all.at[me], part_sem.at[4], part_sem.at[5], "shard", to)
    wait(total_all.at[pl.ds(0, parts - 1)], part_sem.at[5])

    step = jnp.full((1, 1), step_ref[0], jnp.int32).astype(jnp.float32)
    rate = 1.0 / jnp.sqrt(jnp.maximum(step, 10000.0))
    squares = total_all[0, mats : mats + 1, :]
    for s in range(1, parts):
        squares += total_all[s, mats : mats + 1, :]
    for m in range(mats):
        count = row_counts[m]
        average = total[2 * mats : 2 * mats + 1, m : m + 1] / count
        clip = jnp.maximum(1.0, jnp.sqrt(average * squares[:, m : m + 1] / (count * width)))
        gain = jnp.sqrt(average) * rate / clip
        for s in range(parts):
            span = slice(s * cut, (s + 1) * cut)
            cols = total_all[s, m : m + 1, :]
            cols_ref[m : m + 1, span] = cols
            factor[m, :, span] = jnp.broadcast_to(lax.rsqrt(cols) * gain, (CHUNK, cut))

    unroll = largest(4, slot_count)

    def update(u):
        k, c = u // col_groups, u % col_groups
        if c == 0:
            param_load(k).wait()

        def slot(j, carry):
            m = jnp.minimum(ids[j], mats - 1)
            scale = scale_buf[k, j]
            for s in range(parts):
                span = slice(s * cut + c * 128, s * cut + (c + 1) * 128)
                new = param_buf[k, j, :, span].astype(jnp.float32) - grad_buf[k, j, :, span] * scale * factor[m, :, span]
                send_buf[u, s, j] = new.astype(send_buf.dtype)
            return carry

        lax.fori_loop(0, slot_count, slot, 0, unroll=unroll)
        spot = pl.ds(me * slot_count, slot_count)
        for core in (1, 0):
            for step in range(parts // 2):
                to = lax.rem(me // 2 + step, parts // 2) * 2 + core

                @pl.when(to != me)
                def _():
                    send(send_buf.at[u, to], recv_bufs[u].at[spot], cross_send.at[u], cross_recv.at[u], "shard", to)

        pltpu.make_async_copy(send_buf.at[u, me], recv_bufs[u].at[spot], cross_recv.at[u]).start()

    def own(u):
        wait(recv_bufs[u], cross_recv.at[u])

        def pick(b, carry):
            picked[u, b] = recv_bufs[u][spots[b]]
            return carry

        lax.fori_loop(0, blocks, pick, 0, unroll=8)

        @pl.when(z < copies - 1)
        def _():
            send(picked.at[u], temp_ref.at[z, u], line_send.at[0, 0], line_recv.at[0, 0, u], "dp", z + 1)

        @pl.when(z > 0)
        def _():
            send(picked.at[u], temp_ref.at[z, u], line_send.at[1, 0], line_recv.at[1, 0, u], "dp", z - 1)

        pltpu.make_async_copy(picked.at[u], temp_ref.at[z, u], own_sem).start()

    def pass_on(h, u, source, side, to, last):
        block = temp_ref.at[source, u]
        wait(block, line_recv.at[side, h - 1, u])
        if h == copies - 3 and u >= units - tail:
            @pl.when(last)
            def _():
                send(block, late_ref.at[u - units + tail], line_send.at[side, h], line_recv.at[side, h, u], "dp", to)

            @pl.when(jnp.logical_not(last))
            def _():
                send(block, block, line_send.at[side, h], line_recv.at[side, h, u], "dp", to)
        else:
            send(block, block, line_send.at[side, h], line_recv.at[side, h, u], "dp", to)

    def forward(h, u):
        if h == copies - 2 and u >= units - tail:
            return

        @pl.when((z >= h) & (z < copies - 1))
        def _():
            pass_on(h, u, z - h, 0, z + 1, z == copies - 3)

        @pl.when((z + h < copies) & (z > 0))
        def _():
            pass_on(h, u, z + h, 1, z - 1, z == 2)

    early = min(units, 8)
    for u in range(early):
        update(u)
    later = list(range(early, units))
    for i in range(units + copies - 2):
        if i < units:
            own(i)
        for u in later[:4]:
            update(u)
        later = later[4:]
        for h in range(1, copies - 1):
            if 0 <= i - h < units:
                forward(h, i - h)

    for h in range(1, copies):
        for u in range(units - tail if h == copies - 1 else units):
            @pl.when(z == copies - 1)
            def _():
                wait(temp_ref.at[z - h, u], line_recv.at[0, h - 1, u])

            @pl.when(z == 0)
            def _():
                wait(temp_ref.at[z + h, u], line_recv.at[1, h - 1, u])

    for t in range(tail):
        @pl.when(z == copies - 2)
        def _():
            wait(late_ref.at[t], line_recv.at[0, copies - 3, units - tail + t])

        @pl.when(z == 1)
        def _():
            wait(late_ref.at[t], line_recv.at[1, copies - 3, units - tail + t])

    for h in range(copies - 1):
        sent = temp_ref.at[0, pl.ds(0, units - tail if h == copies - 2 else units)]

        @pl.when((z >= h) & (z < copies - 1))
        def _():
            wait(sent, line_send.at[0, h])

        @pl.when((z + h < copies) & (z > 0))
        def _():
            wait(sent, line_send.at[1, h])

    wait(temp_ref.at[0], own_sem)
    for u in range(units):
        wait(send_buf.at[u, pl.ds(0, parts - 1)], cross_send.at[u])
    wait(part_in.at[pl.ds(0, parts - 1)], part_sem.at[0])
    wait(part_all.at[pl.ds(0, copies - 1)], part_sem.at[2])
    wait(total_all.at[pl.ds(0, parts - 1)], part_sem.at[4])


def late_source(copies):
    z = lax.axis_index("dp")
    return jnp.where(z >= copies - 2, 0, jnp.where(z <= 1, copies - 1, copies))


def place_kernel(tail, cols_in, rows_in, in_ref, late_ref, cols_out, rows_out, out_ref, buf, group_load, group_store, load_sem, store_sem, late_load, late_store):
    copies, row_groups = buf.shape[0], buf.shape[1]
    units = in_ref.shape[1]
    col_groups = units // row_groups
    skip = late_source(copies)
    z = lax.axis_index("dp")
    inner = (z == 1) | (z == copies - 2)
    cols_out[...] = cols_in[...]
    rows_out[...] = rows_in[...]
    full = (units - tail) // col_groups
    groups = [(k, d) for k in range(full) for d in range(copies)]
    singles = [(u, d) for u in range(full * col_groups, units) for d in range(copies)]

    def load(u, d, sem):
        k, c = u // col_groups, u % col_groups
        return pltpu.make_async_copy(in_ref.at[d, u], buf.at[d, k, :, :, c * 128 : (c + 1) * 128], sem)

    def store(u, d):
        k, span = u // col_groups, slice(u % col_groups * 128, (u % col_groups + 1) * 128)
        return pltpu.make_async_copy(buf.at[d, k, :, :, span], out_ref.at[:, d, k, :, span], store_sem.at[d, u])

    def group_copy(k, d):
        return pltpu.make_async_copy(buf.at[d, k], out_ref.at[:, d, k], group_store.at[d, k])

    def each(u, d, work):
        if u < units - tail:
            work()
        else:
            pl.when(d != skip)(work)

    for k, d in groups:
        for c in range(col_groups):
            load(k * col_groups + c, d, group_load.at[d, k]).start()
    def load_late(u):
        k, c = u // col_groups, u % col_groups
        return pltpu.make_async_copy(late_ref.at[u - units + tail], buf.at[skip, k, :, :, c * 128 : (c + 1) * 128], late_load.at[u - units + tail])

    def store_late(u):
        k, span = u // col_groups, slice(u % col_groups * 128, (u % col_groups + 1) * 128)
        return pltpu.make_async_copy(buf.at[skip, k, :, :, span], out_ref.at[:, skip, k, :, span], late_store.at[u - units + tail])

    late_units = range(units - tail, units)
    for u, d in singles:
        each(u, d, lambda: load(u, d, load_sem.at[d, u]).start())

    @pl.when(inner)
    def _():
        for u in late_units:
            load_late(u).start()

    for k, d in groups:
        wait(buf.at[d, k], group_load.at[d, k])
        group_copy(k, d).start()
    for u, d in singles:
        def move():
            load(u, d, load_sem.at[d, u]).wait()
            store(u, d).start()

        each(u, d, move)

    @pl.when(inner)
    def _():
        for u in late_units:
            load_late(u).wait()
            store_late(u).start()

    for k, d in groups:
        group_copy(k, d).wait()
    for u, d in singles:
        each(u, d, lambda: store(u, d).wait())

    @pl.when(inner)
    def _():
        for u in late_units:
            store_late(u).wait()


def place_late_kernel(landed_ref, old_ref, out_ref, store_sem):
    tail = landed_ref.shape[0]
    copies, row_groups = out_ref.shape[1], out_ref.shape[2]
    col_groups = out_ref.shape[4] // 128
    z = lax.axis_index("dp")
    skip = late_source(copies)

    def store(t):
        u = row_groups * col_groups - tail + t
        k, span = u // col_groups, slice(u % col_groups * 128, (u % col_groups + 1) * 128)
        return pltpu.make_async_copy(landed_ref.at[t], out_ref.at[:, skip, k, :, span], store_sem.at[t])

    @pl.when((z == 0) | (z == copies - 1))
    def _():
        for t in range(tail):
            store(t).start()
        for t in range(tail):
            store(t).wait()


def body(parts, grad, param, row_state, col_state, block_start, block_matrix, step):
    slot_count, height, width = grad.shape
    mats = col_state.shape[0]
    total_blocks = block_matrix.shape[0]
    group = largest(4, slot_count)
    steps = slot_count // group
    chunks = height // CHUNK
    cut = width // parts
    copies = lax.axis_size("dp")
    assert copies > 3
    units = chunks * (cut // 128)
    tail = min(2, units - 1)
    row_counts = (float(D), float(D), float(FF))

    smem = pl.BlockSpec(memory_space=pltpu.SMEM)
    vmem = pl.BlockSpec(memory_space=pltpu.VMEM)
    hbm = pl.BlockSpec(memory_space=pl.ANY)
    dma = pltpu.SemaphoreType.DMA

    new_cols, new_rows, temp, late = pl.pallas_call(
        functools.partial(main_kernel, mats, group, row_counts),
        in_specs=[smem, smem, smem, vmem, vmem, hbm, hbm],
        out_specs=[vmem, vmem, hbm, hbm],
        out_shape=[
            jax.ShapeDtypeStruct((mats, width), jnp.float32),
            jax.ShapeDtypeStruct((height, slot_count), jnp.float32),
            jax.ShapeDtypeStruct((copies, units, total_blocks, CHUNK, 128), jnp.bfloat16),
            jax.ShapeDtypeStruct((tail, total_blocks, CHUNK, 128), jnp.bfloat16),
        ],
        scratch_shapes=[
            pltpu.SMEM((slot_count,), jnp.int32),
            pltpu.SMEM((total_blocks,), jnp.int32),
            pltpu.VMEM((8, width), jnp.float32),
            pltpu.VMEM((chunks, slot_count, CHUNK, width), jnp.float32),
            pltpu.VMEM((chunks, slot_count, CHUNK, width), jnp.bfloat16),
            pltpu.VMEM((chunks, slot_count, CHUNK, 128), jnp.float32),
            pltpu.VMEM((units, parts, slot_count, CHUNK, 128), jnp.bfloat16),
            pltpu.VMEM((units, total_blocks, CHUNK, 128), jnp.bfloat16),
            pltpu.VMEM((mats, CHUNK, width), jnp.float32),
            pltpu.VMEM((parts, 8, cut), jnp.float32),
            pltpu.VMEM((copies, 8, cut), jnp.float32),
            pltpu.VMEM((parts, mats + 1, cut), jnp.float32),
            pltpu.VMEM((mats, CHUNK, width), jnp.float32),
            pltpu.VMEM((mats, CHUNK, width), jnp.float32),
            pltpu.VMEM((mats, CHUNK, 128), jnp.float32),
            dma((steps,)),
            dma((chunks,)),
            dma((6,)),
            dma((units,)),
            dma((units,)),
            dma((2, copies - 1)),
            dma((2, copies - 1, units)),
            dma(()),
        ]
        + [pltpu.VMEM((parts * slot_count, CHUNK, 128), jnp.bfloat16) for _ in range(units)],
        compiler_params=pltpu.CompilerParams(
            collective_id=0, has_side_effects=True, vmem_limit_bytes=63 * 2**20
        ),
        cost_estimate=pl.CostEstimate(flops=grad.size * 6, bytes_accessed=grad.size * 8, transcendentals=0),
        name="main",
    )(block_start, block_matrix, step, col_state, row_state.T, grad, param)

    landed = lax.ppermute(late, "dp", [(copies - 2, copies - 1), (1, 0)])
    size = total_blocks * copies * height * cut
    placed_shape = jax.ShapeDtypeStruct((total_blocks, copies, chunks, CHUNK, cut), jnp.bfloat16)
    new_cols, new_rows, placed = pl.pallas_call(
        functools.partial(place_kernel, tail),
        in_specs=[vmem, vmem, hbm, hbm],
        out_specs=[vmem, vmem, hbm],
        out_shape=[
            jax.ShapeDtypeStruct((mats, width), jnp.float32),
            jax.ShapeDtypeStruct((height, slot_count), jnp.float32),
            placed_shape,
        ],
        scratch_shapes=[
            pltpu.VMEM((copies, chunks, total_blocks, CHUNK, cut), jnp.bfloat16),
            dma((copies, chunks)),
            dma((copies, chunks)),
            dma((copies, units)),
            dma((copies, units)),
            dma((tail,)),
            dma((tail,)),
        ],
        compiler_params=pltpu.CompilerParams(vmem_limit_bytes=60 * 2**20),
        cost_estimate=pl.CostEstimate(flops=size * 10, bytes_accessed=4 * size, transcendentals=0),
        name="place",
    )(new_cols, new_rows, temp, late)
    placed = pl.pallas_call(
        place_late_kernel,
        in_specs=[hbm, hbm],
        out_specs=hbm,
        out_shape=placed_shape,
        input_output_aliases={1: 0},
        scratch_shapes=[
            dma((tail,)),
        ],
        compiler_params=pltpu.CompilerParams(vmem_limit_bytes=4 * 2**20),
        cost_estimate=pl.CostEstimate(flops=size, bytes_accessed=size, transcendentals=0),
        name="place_late",
    )(landed, placed)
    new_params = placed.reshape(total_blocks * copies * height, cut)
    return new_params, new_rows.T, new_cols


def solution(mesh):
    return jax.shard_map(
        functools.partial(body, mesh.shape["shard"]),
        mesh=mesh,
        in_specs=(
            P("shard", "dp", None),
            P("shard", "dp", None),
            P("shard", "dp"),
            P(),
            P(),
            P(),
            P(),
        ),
        out_specs=(P(None, "shard"), P("shard", "dp"), P()),
        check_vma=False,
    )
```

```python
import functools

import jax
import jax.numpy as jnp
from jax import lax
from jax.experimental import pallas as pl
from jax.experimental.pallas import tpu as pltpu
from jax.sharding import PartitionSpec as P

D = 4096
FF = 10240
MATS = 3
CHUNK = 8


def largest(limit, count):
    return max(n for n in range(1, limit + 1) if count % n == 0)


def wait(ref, sem):
    pltpu.make_async_copy(ref, ref, sem).wait()


def first_and_owned(start_ref, blocks):
    parts = start_ref.shape[0]
    me = lax.axis_index("shard")
    first = start_ref[me]
    end = jnp.where(me == parts - 1, blocks, start_ref[jnp.minimum(me + 1, parts - 1)])
    return first, end - first


def decay_of(step_ref, shape):
    return jnp.exp(-0.8 * jnp.log(jnp.full(shape, step_ref[0], jnp.int32).astype(jnp.float32)))


def main_kernel(mats, group, row_counts, start_ref, matrix_ref, step_ref, state_ref, row_state_ref, grad_ref, param_ref, cols_out, rows_out, temp_ref, late_ref, *scratch):
    (ids, spots, sums_ref, grad_buf, param_buf, scale_buf, send_buf, picked, factor, part_in, part_all, total_all) = scratch[:12]
    (cols_acc, weighted_acc, rows_acc, grad_sem, param_sem, part_sem, cross_send, cross_recv, line_send, line_recv, own_sem) = scratch[12:23]
    (cols_ref, rows_ref, small_sem) = scratch[23:26]
    recv_bufs = scratch[26:]
    small_stores = [
        pltpu.make_async_copy(rows_ref, rows_out, small_sem.at[2]),
        pltpu.make_async_copy(cols_ref, cols_out, small_sem.at[3]),
    ]
    tail = late_ref.shape[0]
    parts, copies = lax.axis_size("shard"), lax.axis_size("dp")
    me, z = lax.axis_index("shard"), lax.axis_index("dp")
    row_groups, slot_count, _, width = grad_buf.shape
    units = len(recv_bufs)
    cut = width // parts
    col_groups = units // row_groups
    blocks = picked.shape[1]
    def param_load(k):
        rows = pl.ds(k * CHUNK, CHUNK)
        return pltpu.make_async_copy(param_ref.at[:, rows, :], param_buf.at[k], param_sem.at[k])

    def send(src, dst, send_sem, recv_sem, axis, to):
        pltpu.make_async_remote_copy(
            src_ref=src,
            dst_ref=dst,
            send_sem=send_sem,
            recv_sem=recv_sem,
            device_id={axis: to},
            device_id_type=pl.DeviceIdType.MESH,
        ).start()

    for i in range(slot_count // group):
        slots = pl.ds(i * group, group)
        for k in range(row_groups):
            rows = pl.ds(k * CHUNK, CHUNK)
            pltpu.make_async_copy(grad_ref.at[slots, rows, :], grad_buf.at[k, slots], grad_sem.at[i]).start()

    barrier = pltpu.get_barrier_semaphore()
    for axis, at, size in (("shard", me, parts), ("dp", z, copies)):
        for step in range(1, size):
            peer = lax.rem(at + step, size)
            pl.semaphore_signal(barrier, inc=1, device_id={axis: peer}, device_id_type=pl.DeviceIdType.MESH)

    first, owned = first_and_owned(start_ref, blocks)

    def note_id(j, carry):
        ids[j] = jnp.where(j < owned, matrix_ref[jnp.minimum(first + j, blocks - 1)], mats)
        return carry

    lax.fori_loop(0, slot_count, note_id, 0)

    decay = decay_of(step_ref, (1, 1))
    cols_acc[...] = jnp.zeros_like(cols_acc)
    weighted_acc[...] = jnp.zeros_like(weighted_acc)
    rows_acc[...] = jnp.zeros_like(rows_acc)
    rows_ref[...] = jnp.zeros_like(rows_ref)
    lane = lax.broadcasted_iota(jnp.int32, (CHUNK, slot_count), 1)
    spans = [slice(n, n + 128) for n in range(0, width, 128)]

    def add_to(acc, ms, span, values):
        for n in range(mats):
            acc[n, :, span] += total_of([jnp.where(m == n, value, 0.0) for m, value in zip(ms, values)])

    def total_of(values):
        while len(values) > 1:
            values = [a + b for a, b in zip(values[::2], values[1::2])] + values[len(values) & ~1 :]
        return values[0]

    def work(i, carry):
        wait(grad_buf.at[:, pl.ds(i * group, group)], grad_sem.at[i])
        slots = [i * group + j for j in range(group)]
        ms = [ids[slot] for slot in slots]
        across = [[jnp.zeros((CHUNK, 128), jnp.float32)] * row_groups for _ in slots]
        for span in spans:
            totals = []
            for j, slot in enumerate(slots):
                tiles = [grad_buf[k, slot, :, span] for k in range(row_groups)]
                tiles = [tile * tile for tile in tiles]
                across[j] = [a + b for a, b in zip(across[j], tiles)]
                totals.append(total_of(tiles))
            add_to(cols_acc, ms, span, totals)
        inverses = []
        for k in range(row_groups):
            at = slice(k * CHUNK, (k + 1) * CHUNK)
            found = []
            for j, slot in enumerate(slots):
                here = lane == slot
                state = jnp.sum(jnp.where(here, row_state_ref[at, :], 0.0), axis=1, keepdims=True)
                rows = (1.0 - decay) * state + decay * (jnp.sum(across[j][k], axis=1, keepdims=True) / width)
                rows_ref[at, :] = jnp.where(here & (ms[j] < mats), rows, rows_ref[at, :])
                rows = jnp.broadcast_to(rows, (CHUNK, 128))
                scale_buf[k, slot] = lax.rsqrt(rows)
                found.append(rows)
            add_to(rows_acc, ms, slice(0, 128), found)
            inverses.append([1.0 / rows for rows in found])
        for span in spans:
            totals = []
            for j, slot in enumerate(slots):
                tiles = [grad_buf[k, slot, :, span] for k in range(row_groups)]
                totals.append(total_of([tile * tile * inverses[k][j] for k, tile in enumerate(tiles)]))
            add_to(weighted_acc, ms, span, totals)
        return carry

    lax.fori_loop(0, slot_count // group, work, 0)
    for k in range(row_groups):
        param_load(k).start()
    for m in range(mats):
        sums_ref[m : m + 1, :] = jnp.sum(cols_acc[m], axis=0, keepdims=True)
        sums_ref[mats + m : mats + m + 1, :] = jnp.sum(weighted_acc[m], axis=0, keepdims=True)
    spot = lax.broadcasted_iota(jnp.int32, (1, width), 1) % cut
    rest = jnp.zeros((1, width), jnp.float32)
    for m in range(mats):
        rest = jnp.where(spot == m, jnp.sum(rows_acc[m], axis=0, keepdims=True)[:, 0:1], rest)
    sums_ref[2 * mats :, :] = jnp.broadcast_to(rest, (8 - 2 * mats, width))
    pl.semaphore_wait(barrier, parts + copies - 2)

    for step in range(1, parts):
        to = lax.rem(me + step, parts)
        span = pl.ds(pl.multiple_of(to * cut, 128), cut)
        send(sums_ref.at[:, span], part_in.at[me], part_sem.at[0], part_sem.at[1], "shard", to)
    mine = pl.ds(pl.multiple_of(me * cut, 128), cut)
    pltpu.make_async_copy(sums_ref.at[:, mine], part_in.at[me], part_sem.at[1]).start()

    def note_spot(b, carry):
        shift = jnp.int32(0)
        for s in range(1, parts):
            shift = jnp.where(b >= start_ref[s], s * slot_count - start_ref[s], shift)
        spots[b] = jnp.minimum(b + shift, parts * slot_count - 1)
        return carry

    lax.fori_loop(0, blocks, note_spot, 0)
    wait(part_in, part_sem.at[1])
    part_all[z] = jnp.sum(part_in[...], axis=0)
    for step in range(1, copies):
        to = lax.rem(z + step, copies)
        send(part_all.at[z], part_all.at[z], part_sem.at[2], part_sem.at[3], "dp", to)
    wait(part_all.at[pl.ds(0, copies - 1)], part_sem.at[3])
    total = jnp.sum(part_all[...], axis=0)
    lanes = lax.broadcasted_iota(jnp.int32, (1, cut), 1)
    partial = jnp.zeros((1, cut), jnp.float32)
    for m in range(mats):
        cols = (1.0 - decay) * state_ref[m : m + 1, mine] + decay * (total[m : m + 1] / row_counts[m])
        total_all[me, m : m + 1, :] = cols
        partial = jnp.where(lanes == m, jnp.sum(total[mats + m : mats + m + 1] / cols, axis=1, keepdims=True), partial)
    total_all[me, mats : mats + 1, :] = partial
    for step in range(1, parts):
        to = lax.rem(me + step, parts)
        send(total_all.at[me], total_all.at[me], part_sem.at[4], part_sem.at[5], "shard", to)
    wait(total_all.at[pl.ds(0, parts - 1)], part_sem.at[5])

    step = jnp.full((1, 1), step_ref[0], jnp.int32).astype(jnp.float32)
    rate = 1.0 / jnp.sqrt(jnp.maximum(step, 10000.0))
    squares = total_all[0, mats : mats + 1, :]
    for s in range(1, parts):
        squares += total_all[s, mats : mats + 1, :]
    for m in range(mats):
        count = row_counts[m]
        average = total[2 * mats : 2 * mats + 1, m : m + 1] / count
        clip = jnp.maximum(1.0, jnp.sqrt(average * squares[:, m : m + 1] / (count * width)))
        gain = jnp.sqrt(average) * rate / clip
        for s in range(parts):
            span = slice(s * cut, (s + 1) * cut)
            cols = total_all[s, m : m + 1, :]
            cols_ref[m : m + 1, span] = cols
            factor[m, :, span] = jnp.broadcast_to(lax.rsqrt(cols) * gain, (CHUNK, cut))

    unroll = largest(4, slot_count)

    def update(u):
        k, c = u // col_groups, u % col_groups
        if c == 0:
            param_load(k).wait()

        spot = pl.ds(me * slot_count, slot_count)
        for core in (1, 0):

            def slot(j, carry):
                m = jnp.minimum(ids[j], mats - 1)
                scale = scale_buf[k, j]
                for s in range(core, parts, 2):
                    span = slice(s * cut + c * 128, s * cut + (c + 1) * 128)
                    new = param_buf[k, j, :, span].astype(jnp.float32) - grad_buf[k, j, :, span] * scale * factor[m, :, span]
                    send_buf[u, s, j] = new.astype(send_buf.dtype)
                return carry

            lax.fori_loop(0, slot_count, slot, 0, unroll=unroll)
            for step in range(parts // 2):
                to = lax.rem(me // 2 + step, parts // 2) * 2 + core

                @pl.when(to != me)
                def _():
                    send(send_buf.at[u, to], recv_bufs[u].at[spot], cross_send.at[u], cross_recv.at[u], "shard", to)

        pltpu.make_async_copy(send_buf.at[u, me], recv_bufs[u].at[spot], cross_recv.at[u]).start()

    def own(u):
        wait(recv_bufs[u], cross_recv.at[u])

        def pick(b, carry):
            picked[u, b] = recv_bufs[u][spots[b]]
            return carry

        lax.fori_loop(0, blocks, pick, 0, unroll=8)

        @pl.when(z < copies - 1)
        def _():
            send(picked.at[u], temp_ref.at[z, u], line_send.at[0, 0], line_recv.at[0, 0, u], "dp", z + 1)

        @pl.when(z > 0)
        def _():
            send(picked.at[u], temp_ref.at[z, u], line_send.at[1, 0], line_recv.at[1, 0, u], "dp", z - 1)

        pltpu.make_async_copy(picked.at[u], temp_ref.at[z, u], own_sem).start()

    def pass_on(h, u, source, side, to, last):
        block = temp_ref.at[source, u]
        wait(block, line_recv.at[side, h - 1, u])
        if h == copies - 3 and u >= units - tail:
            @pl.when(last)
            def _():
                send(block, late_ref.at[u - units + tail], line_send.at[side, h], line_recv.at[side, h, u], "dp", to)

            @pl.when(jnp.logical_not(last))
            def _():
                send(block, block, line_send.at[side, h], line_recv.at[side, h, u], "dp", to)
        else:
            send(block, block, line_send.at[side, h], line_recv.at[side, h, u], "dp", to)

    def forward(h, u):
        if h == copies - 2 and u >= units - tail:
            return

        @pl.when((z >= h) & (z < copies - 1))
        def _():
            pass_on(h, u, z - h, 0, z + 1, z == copies - 3)

        @pl.when((z + h < copies) & (z > 0))
        def _():
            pass_on(h, u, z + h, 1, z - 1, z == 2)

    early = min(units, 8)
    for u in range(early):
        update(u)
        if u == 0:
            for copy in small_stores:
                copy.start()
    later = list(range(early, units))
    for i in range(units + copies - 2):
        if i < units:
            own(i)
        for u in later[:4]:
            update(u)
        later = later[4:]
        for h in range(1, copies - 1):
            if 0 <= i - h < units:
                forward(h, i - h)

    for h in range(1, copies):
        for u in range(units - tail if h == copies - 1 else units):
            @pl.when(z == copies - 1)
            def _():
                wait(temp_ref.at[z - h, u], line_recv.at[0, h - 1, u])

            @pl.when(z == 0)
            def _():
                wait(temp_ref.at[z + h, u], line_recv.at[1, h - 1, u])

    for t in range(tail):
        @pl.when(z == copies - 2)
        def _():
            wait(late_ref.at[t], line_recv.at[0, copies - 3, units - tail + t])

        @pl.when(z == 1)
        def _():
            wait(late_ref.at[t], line_recv.at[1, copies - 3, units - tail + t])

    for h in range(copies - 1):
        sent = temp_ref.at[0, pl.ds(0, units - tail if h == copies - 2 else units)]

        @pl.when((z >= h) & (z < copies - 1))
        def _():
            wait(sent, line_send.at[0, h])

        @pl.when((z + h < copies) & (z > 0))
        def _():
            wait(sent, line_send.at[1, h])

    for copy in small_stores:
        copy.wait()
    wait(temp_ref.at[0], own_sem)
    for u in range(units):
        wait(send_buf.at[u, pl.ds(0, parts - 1)], cross_send.at[u])
    wait(part_in.at[pl.ds(0, parts - 1)], part_sem.at[0])
    wait(part_all.at[pl.ds(0, copies - 1)], part_sem.at[2])
    wait(total_all.at[pl.ds(0, parts - 1)], part_sem.at[4])


def late_source(copies):
    z = lax.axis_index("dp")
    return jnp.where(z >= copies - 2, 0, jnp.where(z <= 1, copies - 1, copies))


def place_kernel(tail, cols_in, rows_in, in_ref, late_ref, cols_out, rows_out, out_ref, cols_buf, rows_buf, small_sem, buf, group_load, group_store, load_sem, store_sem, late_load, late_store):
    copies, row_groups = buf.shape[0], buf.shape[1]
    units = in_ref.shape[1]
    col_groups = units // row_groups
    skip = late_source(copies)
    z = lax.axis_index("dp")
    inner = (z == 1) | (z == copies - 2)
    small_loads = [
        pltpu.make_async_copy(cols_in, cols_buf, small_sem.at[0]),
        pltpu.make_async_copy(rows_in, rows_buf, small_sem.at[1]),
    ]
    small_stores = [
        pltpu.make_async_copy(cols_buf, cols_out, small_sem.at[2]),
        pltpu.make_async_copy(rows_buf, rows_out, small_sem.at[3]),
    ]
    for copy in small_loads:
        copy.start()
    full = (units - tail) // col_groups
    groups = [(k, d) for k in range(full) for d in range(copies)]
    singles = [(u, d) for u in range(full * col_groups, units) for d in range(copies)]

    def load(u, d, sem):
        k, c = u // col_groups, u % col_groups
        return pltpu.make_async_copy(in_ref.at[d, u], buf.at[d, k, :, :, c * 128 : (c + 1) * 128], sem)

    def store(u, d):
        k, span = u // col_groups, slice(u % col_groups * 128, (u % col_groups + 1) * 128)
        return pltpu.make_async_copy(buf.at[d, k, :, :, span], out_ref.at[:, d, k, :, span], store_sem.at[d, u])

    def group_copy(k, d):
        return pltpu.make_async_copy(buf.at[d, k], out_ref.at[:, d, k], group_store.at[d, k])

    def each(u, d, work):
        if u < units - tail:
            work()
        else:
            pl.when(d != skip)(work)

    for k, d in groups:
        for c in range(col_groups):
            load(k * col_groups + c, d, group_load.at[d, k]).start()
    def load_late(u):
        k, c = u // col_groups, u % col_groups
        return pltpu.make_async_copy(late_ref.at[u - units + tail], buf.at[skip, k, :, :, c * 128 : (c + 1) * 128], late_load.at[u - units + tail])

    def store_late(u):
        k, span = u // col_groups, slice(u % col_groups * 128, (u % col_groups + 1) * 128)
        return pltpu.make_async_copy(buf.at[skip, k, :, :, span], out_ref.at[:, skip, k, :, span], late_store.at[u - units + tail])

    late_units = range(units - tail, units)
    for u, d in singles:
        each(u, d, lambda: load(u, d, load_sem.at[d, u]).start())

    @pl.when(inner)
    def _():
        for u in late_units:
            load_late(u).start()

    for a, b in zip(small_loads, small_stores):
        a.wait()
        b.start()
    for k, d in groups:
        wait(buf.at[d, k], group_load.at[d, k])
        group_copy(k, d).start()
    for u, d in singles:
        def move():
            load(u, d, load_sem.at[d, u]).wait()
            store(u, d).start()

        each(u, d, move)

    @pl.when(inner)
    def _():
        for u in late_units:
            load_late(u).wait()
            store_late(u).start()

    for copy in small_stores:
        copy.wait()
    for k, d in groups:
        group_copy(k, d).wait()
    for u, d in singles:
        each(u, d, lambda: store(u, d).wait())

    @pl.when(inner)
    def _():
        for u in late_units:
            store_late(u).wait()


def place_late_kernel(landed_ref, old_ref, out_ref, store_sem):
    tail = landed_ref.shape[0]
    copies, row_groups = out_ref.shape[1], out_ref.shape[2]
    col_groups = out_ref.shape[4] // 128
    z = lax.axis_index("dp")
    skip = late_source(copies)

    def store(t):
        u = row_groups * col_groups - tail + t
        k, span = u // col_groups, slice(u % col_groups * 128, (u % col_groups + 1) * 128)
        return pltpu.make_async_copy(landed_ref.at[t], out_ref.at[:, skip, k, :, span], store_sem.at[t])

    @pl.when((z == 0) | (z == copies - 1))
    def _():
        for t in range(tail):
            store(t).start()
        for t in range(tail):
            store(t).wait()


def body(parts, grad, param, row_state, col_state, block_start, block_matrix, step):
    slot_count, height, width = grad.shape
    mats = col_state.shape[0]
    total_blocks = block_matrix.shape[0]
    group = largest(4, slot_count)
    steps = slot_count // group
    chunks = height // CHUNK
    cut = width // parts
    copies = lax.axis_size("dp")
    assert copies > 3
    units = chunks * (cut // 128)
    tail = min(2, units - 1)
    row_counts = (float(D), float(D), float(FF))

    smem = pl.BlockSpec(memory_space=pltpu.SMEM)
    vmem = pl.BlockSpec(memory_space=pltpu.VMEM)
    hbm = pl.BlockSpec(memory_space=pl.ANY)
    dma = pltpu.SemaphoreType.DMA

    new_cols, new_rows, temp, late = pl.pallas_call(
        functools.partial(main_kernel, mats, group, row_counts),
        in_specs=[smem, smem, smem, vmem, vmem, hbm, hbm],
        out_specs=[hbm, hbm, hbm, hbm],
        out_shape=[
            jax.ShapeDtypeStruct((mats, width), jnp.float32),
            jax.ShapeDtypeStruct((height, slot_count), jnp.float32),
            jax.ShapeDtypeStruct((copies, units, total_blocks, CHUNK, 128), jnp.bfloat16),
            jax.ShapeDtypeStruct((tail, total_blocks, CHUNK, 128), jnp.bfloat16),
        ],
        scratch_shapes=[
            pltpu.SMEM((slot_count,), jnp.int32),
            pltpu.SMEM((total_blocks,), jnp.int32),
            pltpu.VMEM((8, width), jnp.float32),
            pltpu.VMEM((chunks, slot_count, CHUNK, width), jnp.float32),
            pltpu.VMEM((chunks, slot_count, CHUNK, width), jnp.bfloat16),
            pltpu.VMEM((chunks, slot_count, CHUNK, 128), jnp.float32),
            pltpu.VMEM((units, parts, slot_count, CHUNK, 128), jnp.bfloat16),
            pltpu.VMEM((units, total_blocks, CHUNK, 128), jnp.bfloat16),
            pltpu.VMEM((mats, CHUNK, width), jnp.float32),
            pltpu.VMEM((parts, 8, cut), jnp.float32),
            pltpu.VMEM((copies, 8, cut), jnp.float32),
            pltpu.VMEM((parts, mats + 1, cut), jnp.float32),
            pltpu.VMEM((mats, CHUNK, width), jnp.float32),
            pltpu.VMEM((mats, CHUNK, width), jnp.float32),
            pltpu.VMEM((mats, CHUNK, 128), jnp.float32),
            dma((steps,)),
            dma((chunks,)),
            dma((6,)),
            dma((units,)),
            dma((units,)),
            dma((2, copies - 1)),
            dma((2, copies - 1, units)),
            dma(()),
            pltpu.VMEM((mats, width), jnp.float32),
            pltpu.VMEM((height, slot_count), jnp.float32),
            dma((4,)),
        ]
        + [pltpu.VMEM((parts * slot_count, CHUNK, 128), jnp.bfloat16) for _ in range(units)],
        compiler_params=pltpu.CompilerParams(
            collective_id=0, has_side_effects=True, vmem_limit_bytes=63 * 2**20
        ),
        cost_estimate=pl.CostEstimate(flops=grad.size * 6, bytes_accessed=grad.size * 8, transcendentals=0),
        name="main",
    )(block_start, block_matrix, step, col_state, row_state.T, grad, param)

    landed = lax.ppermute(late, "dp", [(copies - 2, copies - 1), (1, 0)])
    size = total_blocks * copies * height * cut
    placed_shape = jax.ShapeDtypeStruct((total_blocks, copies, chunks, CHUNK, cut), jnp.bfloat16)
    new_cols, new_rows, placed = pl.pallas_call(
        functools.partial(place_kernel, tail),
        in_specs=[hbm, hbm, hbm, hbm],
        out_specs=[hbm, hbm, hbm],
        out_shape=[
            jax.ShapeDtypeStruct((mats, width), jnp.float32),
            jax.ShapeDtypeStruct((height, slot_count), jnp.float32),
            placed_shape,
        ],
        scratch_shapes=[
            pltpu.VMEM((mats, width), jnp.float32),
            pltpu.VMEM((height, slot_count), jnp.float32),
            dma((4,)),
            pltpu.VMEM((copies, chunks, total_blocks, CHUNK, cut), jnp.bfloat16),
            dma((copies, chunks)),
            dma((copies, chunks)),
            dma((copies, units)),
            dma((copies, units)),
            dma((tail,)),
            dma((tail,)),
        ],
        compiler_params=pltpu.CompilerParams(vmem_limit_bytes=60 * 2**20),
        cost_estimate=pl.CostEstimate(flops=size * 10, bytes_accessed=4 * size, transcendentals=0),
        name="place",
    )(new_cols, new_rows, temp, late)
    placed = pl.pallas_call(
        place_late_kernel,
        in_specs=[hbm, hbm],
        out_specs=hbm,
        out_shape=placed_shape,
        input_output_aliases={1: 0},
        scratch_shapes=[
            dma((tail,)),
        ],
        compiler_params=pltpu.CompilerParams(vmem_limit_bytes=4 * 2**20),
        cost_estimate=pl.CostEstimate(flops=size, bytes_accessed=size, transcendentals=0),
        name="place_late",
    )(landed, placed)
    new_params = placed.reshape(total_blocks * copies * height, cut)
    return new_params, new_rows.T, new_cols


def solution(mesh):
    return jax.shard_map(
        functools.partial(body, mesh.shape["shard"]),
        mesh=mesh,
        in_specs=(
            P("shard", "dp", None),
            P("shard", "dp", None),
            P("shard", "dp"),
            P(),
            P(),
            P(),
            P(),
        ),
        out_specs=(P(None, "shard"), P("shard", "dp"), P()),
        check_vma=False,
    )
```

```python
import functools

import jax
import jax.numpy as jnp
from jax import lax
from jax.experimental import pallas as pl
from jax.experimental.pallas import tpu as pltpu
from jax.sharding import PartitionSpec as P

D = 4096
FF = 10240
MATS = 3
CHUNK = 8


def largest(limit, count):
    return max(n for n in range(1, limit + 1) if count % n == 0)


def wait(ref, sem):
    pltpu.make_async_copy(ref, ref, sem).wait()


def first_and_owned(start_ref, blocks):
    parts = start_ref.shape[0]
    me = lax.axis_index("shard")
    first = start_ref[me]
    end = jnp.where(me == parts - 1, blocks, start_ref[jnp.minimum(me + 1, parts - 1)])
    return first, end - first


def decay_of(step_ref, shape):
    return jnp.exp(-0.8 * jnp.log(jnp.full(shape, step_ref[0], jnp.int32).astype(jnp.float32)))


def main_kernel(mats, group, row_counts, start_ref, matrix_ref, step_ref, state_ref, row_state_ref, grad_ref, param_ref, cols_out, rows_out, temp_ref, late_ref, *scratch):
    (ids, spots, sums_ref, grad_buf, param_buf, scale_buf, send_buf, picked, factor, part_in, part_all, total_all) = scratch[:12]
    (cols_acc, weighted_acc, rows_acc, grad_sem, param_sem, part_sem, cross_send, cross_recv, line_send, line_recv, own_sem) = scratch[12:23]
    (cols_ref, rows_ref, small_sem) = scratch[23:26]
    recv_bufs = scratch[26:]
    small_stores = [
        pltpu.make_async_copy(rows_ref, rows_out, small_sem.at[2]),
        pltpu.make_async_copy(cols_ref, cols_out, small_sem.at[3]),
    ]
    tail = late_ref.shape[0]
    parts, copies = lax.axis_size("shard"), lax.axis_size("dp")
    me, z = lax.axis_index("shard"), lax.axis_index("dp")
    row_groups, slot_count, _, width = grad_buf.shape
    units = len(recv_bufs)
    cut = width // parts
    col_groups = units // row_groups
    blocks = picked.shape[1]
    def param_load(k):
        rows = pl.ds(k * CHUNK, CHUNK)
        return pltpu.make_async_copy(param_ref.at[:, rows, :], param_buf.at[k], param_sem.at[k])

    def send(src, dst, send_sem, recv_sem, axis, to):
        pltpu.make_async_remote_copy(
            src_ref=src,
            dst_ref=dst,
            send_sem=send_sem,
            recv_sem=recv_sem,
            device_id={axis: to},
            device_id_type=pl.DeviceIdType.MESH,
        ).start()

    for i in range(slot_count // group):
        slots = pl.ds(i * group, group)
        for k in range(row_groups):
            rows = pl.ds(k * CHUNK, CHUNK)
            pltpu.make_async_copy(grad_ref.at[slots, rows, :], grad_buf.at[k, slots], grad_sem.at[i]).start()

    barrier = pltpu.get_barrier_semaphore()
    for axis, at, size in (("shard", me, parts), ("dp", z, copies)):
        for step in range(1, size):
            peer = lax.rem(at + step, size)
            pl.semaphore_signal(barrier, inc=1, device_id={axis: peer}, device_id_type=pl.DeviceIdType.MESH)

    first, owned = first_and_owned(start_ref, blocks)

    def note_id(j, carry):
        ids[j] = jnp.where(j < owned, matrix_ref[jnp.minimum(first + j, blocks - 1)], mats)
        return carry

    lax.fori_loop(0, slot_count, note_id, 0)

    decay = decay_of(step_ref, (1, 1))
    cols_acc[...] = jnp.zeros_like(cols_acc)
    weighted_acc[...] = jnp.zeros_like(weighted_acc)
    rows_acc[...] = jnp.zeros_like(rows_acc)
    rows_ref[...] = jnp.zeros_like(rows_ref)
    lane = lax.broadcasted_iota(jnp.int32, (CHUNK, slot_count), 1)
    spans = [slice(n, n + 128) for n in range(0, width, 128)]

    def add_to(acc, ms, span, values):
        for n in range(mats):
            acc[n, :, span] += total_of([jnp.where(m == n, value, 0.0) for m, value in zip(ms, values)])

    def total_of(values):
        while len(values) > 1:
            values = [a + b for a, b in zip(values[::2], values[1::2])] + values[len(values) & ~1 :]
        return values[0]

    def work(i, carry):
        wait(grad_buf.at[:, pl.ds(i * group, group)], grad_sem.at[i])
        slots = [i * group + j for j in range(group)]
        ms = [ids[slot] for slot in slots]
        across = [[jnp.zeros((CHUNK, 128), jnp.float32)] * row_groups for _ in slots]
        for span in spans:
            totals = []
            for j, slot in enumerate(slots):
                tiles = [grad_buf[k, slot, :, span] for k in range(row_groups)]
                tiles = [tile * tile for tile in tiles]
                across[j] = [a + b for a, b in zip(across[j], tiles)]
                totals.append(total_of(tiles))
            add_to(cols_acc, ms, span, totals)
        inverses = []
        for k in range(row_groups):
            at = slice(k * CHUNK, (k + 1) * CHUNK)
            found = []
            for j, slot in enumerate(slots):
                here = lane == slot
                state = jnp.sum(jnp.where(here, row_state_ref[at, :], 0.0), axis=1, keepdims=True)
                rows = (1.0 - decay) * state + decay * (jnp.sum(across[j][k], axis=1, keepdims=True) / width)
                rows_ref[at, :] = jnp.where(here & (ms[j] < mats), rows, rows_ref[at, :])
                rows = jnp.broadcast_to(rows, (CHUNK, 128))
                scale_buf[k, slot] = lax.rsqrt(rows)
                found.append(rows)
            add_to(rows_acc, ms, slice(0, 128), found)
            inverses.append([1.0 / rows for rows in found])
        for span in spans:
            totals = []
            for j, slot in enumerate(slots):
                tiles = [grad_buf[k, slot, :, span] for k in range(row_groups)]
                totals.append(total_of([tile * tile * inverses[k][j] for k, tile in enumerate(tiles)]))
            add_to(weighted_acc, ms, span, totals)
        return carry

    lax.fori_loop(0, slot_count // group, work, 0)
    for k in range(row_groups):
        param_load(k).start()
    for m in range(mats):
        sums_ref[m : m + 1, :] = jnp.sum(cols_acc[m], axis=0, keepdims=True)
        sums_ref[mats + m : mats + m + 1, :] = jnp.sum(weighted_acc[m], axis=0, keepdims=True)
    spot = lax.broadcasted_iota(jnp.int32, (1, width), 1) % cut
    rest = jnp.zeros((1, width), jnp.float32)
    for m in range(mats):
        rest = jnp.where(spot == m, jnp.sum(rows_acc[m], axis=0, keepdims=True)[:, 0:1], rest)
    sums_ref[2 * mats :, :] = jnp.broadcast_to(rest, (8 - 2 * mats, width))
    pl.semaphore_wait(barrier, parts + copies - 2)

    for step in range(1, parts):
        to = lax.rem(me + step, parts)
        span = pl.ds(pl.multiple_of(to * cut, 128), cut)
        send(sums_ref.at[:, span], part_in.at[me], part_sem.at[0], part_sem.at[1], "shard", to)
    mine = pl.ds(pl.multiple_of(me * cut, 128), cut)
    pltpu.make_async_copy(sums_ref.at[:, mine], part_in.at[me], part_sem.at[1]).start()

    def note_spot(b, carry):
        shift = jnp.int32(0)
        for s in range(1, parts):
            shift = jnp.where(b >= start_ref[s], s * slot_count - start_ref[s], shift)
        spots[b] = jnp.minimum(b + shift, parts * slot_count - 1)
        return carry

    lax.fori_loop(0, blocks, note_spot, 0)
    wait(part_in, part_sem.at[1])
    part_all[z] = jnp.sum(part_in[...], axis=0)
    for step in range(1, copies):
        to = lax.rem(z + step, copies)
        send(part_all.at[z], part_all.at[z], part_sem.at[2], part_sem.at[3], "dp", to)
    wait(part_all.at[pl.ds(0, copies - 1)], part_sem.at[3])
    total = jnp.sum(part_all[...], axis=0)
    lanes = lax.broadcasted_iota(jnp.int32, (1, cut), 1)
    partial = jnp.zeros((1, cut), jnp.float32)
    for m in range(mats):
        cols = (1.0 - decay) * state_ref[m : m + 1, mine] + decay * (total[m : m + 1] / row_counts[m])
        total_all[me, m : m + 1, :] = cols
        partial = jnp.where(lanes == m, jnp.sum(total[mats + m : mats + m + 1] / cols, axis=1, keepdims=True), partial)
    total_all[me, mats : mats + 1, :] = partial
    for step in range(1, parts):
        to = lax.rem(me + step, parts)
        send(total_all.at[me], total_all.at[me], part_sem.at[4], part_sem.at[5], "shard", to)
    wait(total_all.at[pl.ds(0, parts - 1)], part_sem.at[5])

    step = jnp.full((1, 1), step_ref[0], jnp.int32).astype(jnp.float32)
    rate = 1.0 / jnp.sqrt(jnp.maximum(step, 10000.0))
    squares = total_all[0, mats : mats + 1, :]
    for s in range(1, parts):
        squares += total_all[s, mats : mats + 1, :]
    for m in range(mats):
        count = row_counts[m]
        average = total[2 * mats : 2 * mats + 1, m : m + 1] / count
        clip = jnp.maximum(1.0, jnp.sqrt(average * squares[:, m : m + 1] / (count * width)))
        gain = jnp.sqrt(average) * rate / clip
        for s in range(parts):
            span = slice(s * cut, (s + 1) * cut)
            cols = total_all[s, m : m + 1, :]
            cols_ref[m : m + 1, span] = cols
            factor[m, :, span] = jnp.broadcast_to(lax.rsqrt(cols) * gain, (CHUNK, cut))

    unroll = largest(4, slot_count)

    def update(u):
        k, c = u // col_groups, u % col_groups
        if c == 0:
            param_load(k).wait()

        spot = pl.ds(me * slot_count, slot_count)
        for core in (1, 0):

            def slot(j, carry):
                m = jnp.minimum(ids[j], mats - 1)
                scale = scale_buf[k, j]
                for s in range(core, parts, 2):
                    span = slice(s * cut + c * 128, s * cut + (c + 1) * 128)
                    new = param_buf[k, j, :, span].astype(jnp.float32) - grad_buf[k, j, :, span] * scale * factor[m, :, span]
                    send_buf[u, s, j] = new.astype(send_buf.dtype)
                return carry

            lax.fori_loop(0, slot_count, slot, 0, unroll=unroll)
            for step in range(parts // 2):
                to = lax.rem(me // 2 + step, parts // 2) * 2 + core

                @pl.when(to != me)
                def _():
                    send(send_buf.at[u, to], recv_bufs[u].at[spot], cross_send.at[u], cross_recv.at[u], "shard", to)

        pltpu.make_async_copy(send_buf.at[u, me], recv_bufs[u].at[spot], cross_recv.at[u]).start()

    def own(u):
        wait(recv_bufs[u], cross_recv.at[u])

        def pick(b, carry):
            picked[u, b] = recv_bufs[u][spots[b]]
            return carry

        lax.fori_loop(0, blocks, pick, 0, unroll=8)

        @pl.when(z < copies - 1)
        def _():
            send(picked.at[u], temp_ref.at[z, u], line_send.at[0, 0], line_recv.at[0, 0, u], "dp", z + 1)

        @pl.when(z > 0)
        def _():
            send(picked.at[u], temp_ref.at[z, u], line_send.at[1, 0], line_recv.at[1, 0, u], "dp", z - 1)

        pltpu.make_async_copy(picked.at[u], temp_ref.at[z, u], own_sem).start()

    def pass_on(h, u, source, side, to, last):
        block = temp_ref.at[source, u]
        wait(block, line_recv.at[side, h - 1, u])
        if h == copies - 3 and u >= units - tail:
            @pl.when(last)
            def _():
                send(block, late_ref.at[u - units + tail], line_send.at[side, h], line_recv.at[side, h, u], "dp", to)

            @pl.when(jnp.logical_not(last))
            def _():
                send(block, block, line_send.at[side, h], line_recv.at[side, h, u], "dp", to)
        else:
            send(block, block, line_send.at[side, h], line_recv.at[side, h, u], "dp", to)

    def forward(h, u):
        if h == copies - 2 and u >= units - tail:
            return

        @pl.when((z >= h) & (z < copies - 1))
        def _():
            pass_on(h, u, z - h, 0, z + 1, z == copies - 3)

        @pl.when((z + h < copies) & (z > 0))
        def _():
            pass_on(h, u, z + h, 1, z - 1, z == 2)

    early = min(units, 4)
    for u in range(early):
        update(u)
        if u == 0:
            for copy in small_stores:
                copy.start()
    later = list(range(early, units))
    for i in range(units + copies - 2):
        if i < units:
            own(i)
        for u in later[:4]:
            update(u)
        later = later[4:]
        for h in range(1, copies - 1):
            if 0 <= i - h < units:
                forward(h, i - h)

    for h in range(1, copies):
        for u in range(units - tail if h == copies - 1 else units):
            @pl.when(z == copies - 1)
            def _():
                wait(temp_ref.at[z - h, u], line_recv.at[0, h - 1, u])

            @pl.when(z == 0)
            def _():
                wait(temp_ref.at[z + h, u], line_recv.at[1, h - 1, u])

    for t in range(tail):
        @pl.when(z == copies - 2)
        def _():
            wait(late_ref.at[t], line_recv.at[0, copies - 3, units - tail + t])

        @pl.when(z == 1)
        def _():
            wait(late_ref.at[t], line_recv.at[1, copies - 3, units - tail + t])

    for h in range(copies - 1):
        sent = temp_ref.at[0, pl.ds(0, units - tail if h == copies - 2 else units)]

        @pl.when((z >= h) & (z < copies - 1))
        def _():
            wait(sent, line_send.at[0, h])

        @pl.when((z + h < copies) & (z > 0))
        def _():
            wait(sent, line_send.at[1, h])

    for copy in small_stores:
        copy.wait()
    wait(temp_ref.at[0], own_sem)
    for u in range(units):
        wait(send_buf.at[u, pl.ds(0, parts - 1)], cross_send.at[u])
    wait(part_in.at[pl.ds(0, parts - 1)], part_sem.at[0])
    wait(part_all.at[pl.ds(0, copies - 1)], part_sem.at[2])
    wait(total_all.at[pl.ds(0, parts - 1)], part_sem.at[4])


def late_source(copies):
    z = lax.axis_index("dp")
    return jnp.where(z >= copies - 2, 0, jnp.where(z <= 1, copies - 1, copies))


def place_kernel(tail, cols_in, rows_in, in_ref, late_ref, cols_out, rows_out, out_ref, cols_buf, rows_buf, small_sem, buf, group_load, group_store, load_sem, store_sem, late_load, late_store):
    copies, row_groups = buf.shape[0], buf.shape[1]
    units = in_ref.shape[1]
    col_groups = units // row_groups
    skip = late_source(copies)
    z = lax.axis_index("dp")
    inner = (z == 1) | (z == copies - 2)
    small_loads = [
        pltpu.make_async_copy(cols_in, cols_buf, small_sem.at[0]),
        pltpu.make_async_copy(rows_in, rows_buf, small_sem.at[1]),
    ]
    small_stores = [
        pltpu.make_async_copy(cols_buf, cols_out, small_sem.at[2]),
        pltpu.make_async_copy(rows_buf, rows_out, small_sem.at[3]),
    ]
    for copy in small_loads:
        copy.start()
    full = (units - tail) // col_groups
    groups = [(k, d) for k in range(full) for d in range(copies)]
    singles = [(u, d) for u in range(full * col_groups, units) for d in range(copies)]

    def load(u, d, sem):
        k, c = u // col_groups, u % col_groups
        return pltpu.make_async_copy(in_ref.at[d, u], buf.at[d, k, :, :, c * 128 : (c + 1) * 128], sem)

    def store(u, d):
        k, span = u // col_groups, slice(u % col_groups * 128, (u % col_groups + 1) * 128)
        return pltpu.make_async_copy(buf.at[d, k, :, :, span], out_ref.at[:, d, k, :, span], store_sem.at[d, u])

    def group_copy(k, d):
        return pltpu.make_async_copy(buf.at[d, k], out_ref.at[:, d, k], group_store.at[d, k])

    def each(u, d, work):
        if u < units - tail:
            work()
        else:
            pl.when(d != skip)(work)

    for k, d in groups:
        for c in range(col_groups):
            load(k * col_groups + c, d, group_load.at[d, k]).start()
    def load_late(u):
        k, c = u // col_groups, u % col_groups
        return pltpu.make_async_copy(late_ref.at[u - units + tail], buf.at[skip, k, :, :, c * 128 : (c + 1) * 128], late_load.at[u - units + tail])

    def store_late(u):
        k, span = u // col_groups, slice(u % col_groups * 128, (u % col_groups + 1) * 128)
        return pltpu.make_async_copy(buf.at[skip, k, :, :, span], out_ref.at[:, skip, k, :, span], late_store.at[u - units + tail])

    late_units = range(units - tail, units)
    for u, d in singles:
        each(u, d, lambda: load(u, d, load_sem.at[d, u]).start())

    @pl.when(inner)
    def _():
        for u in late_units:
            load_late(u).start()

    for a, b in zip(small_loads, small_stores):
        a.wait()
        b.start()
    for k, d in groups:
        wait(buf.at[d, k], group_load.at[d, k])
        group_copy(k, d).start()
    for u, d in singles:
        def move():
            load(u, d, load_sem.at[d, u]).wait()
            store(u, d).start()

        each(u, d, move)

    @pl.when(inner)
    def _():
        for u in late_units:
            load_late(u).wait()
            store_late(u).start()

    for copy in small_stores:
        copy.wait()
    for k, d in groups:
        group_copy(k, d).wait()
    for u, d in singles:
        each(u, d, lambda: store(u, d).wait())

    @pl.when(inner)
    def _():
        for u in late_units:
            store_late(u).wait()


def place_late_kernel(landed_ref, old_ref, out_ref, store_sem):
    tail = landed_ref.shape[0]
    copies, row_groups = out_ref.shape[1], out_ref.shape[2]
    col_groups = out_ref.shape[4] // 128
    z = lax.axis_index("dp")
    skip = late_source(copies)

    def store(t):
        u = row_groups * col_groups - tail + t
        k, span = u // col_groups, slice(u % col_groups * 128, (u % col_groups + 1) * 128)
        return pltpu.make_async_copy(landed_ref.at[t], out_ref.at[:, skip, k, :, span], store_sem.at[t])

    @pl.when((z == 0) | (z == copies - 1))
    def _():
        for t in range(tail):
            store(t).start()
        for t in range(tail):
            store(t).wait()


def body(parts, grad, param, row_state, col_state, block_start, block_matrix, step):
    slot_count, height, width = grad.shape
    mats = col_state.shape[0]
    total_blocks = block_matrix.shape[0]
    group = largest(4, slot_count)
    steps = slot_count // group
    chunks = height // CHUNK
    cut = width // parts
    copies = lax.axis_size("dp")
    assert copies > 3
    units = chunks * (cut // 128)
    tail = min(3, units - 1)
    row_counts = (float(D), float(D), float(FF))

    smem = pl.BlockSpec(memory_space=pltpu.SMEM)
    vmem = pl.BlockSpec(memory_space=pltpu.VMEM)
    hbm = pl.BlockSpec(memory_space=pl.ANY)
    dma = pltpu.SemaphoreType.DMA

    new_cols, new_rows, temp, late = pl.pallas_call(
        functools.partial(main_kernel, mats, group, row_counts),
        in_specs=[smem, smem, smem, vmem, vmem, hbm, hbm],
        out_specs=[hbm, hbm, hbm, hbm],
        out_shape=[
            jax.ShapeDtypeStruct((mats, width), jnp.float32),
            jax.ShapeDtypeStruct((height, slot_count), jnp.float32),
            jax.ShapeDtypeStruct((copies, units, total_blocks, CHUNK, 128), jnp.bfloat16),
            jax.ShapeDtypeStruct((tail, total_blocks, CHUNK, 128), jnp.bfloat16),
        ],
        scratch_shapes=[
            pltpu.SMEM((slot_count,), jnp.int32),
            pltpu.SMEM((total_blocks,), jnp.int32),
            pltpu.VMEM((8, width), jnp.float32),
            pltpu.VMEM((chunks, slot_count, CHUNK, width), jnp.float32),
            pltpu.VMEM((chunks, slot_count, CHUNK, width), jnp.bfloat16),
            pltpu.VMEM((chunks, slot_count, CHUNK, 128), jnp.float32),
            pltpu.VMEM((units, parts, slot_count, CHUNK, 128), jnp.bfloat16),
            pltpu.VMEM((units, total_blocks, CHUNK, 128), jnp.bfloat16),
            pltpu.VMEM((mats, CHUNK, width), jnp.float32),
            pltpu.VMEM((parts, 8, cut), jnp.float32),
            pltpu.VMEM((copies, 8, cut), jnp.float32),
            pltpu.VMEM((parts, mats + 1, cut), jnp.float32),
            pltpu.VMEM((mats, CHUNK, width), jnp.float32),
            pltpu.VMEM((mats, CHUNK, width), jnp.float32),
            pltpu.VMEM((mats, CHUNK, 128), jnp.float32),
            dma((steps,)),
            dma((chunks,)),
            dma((6,)),
            dma((units,)),
            dma((units,)),
            dma((2, copies - 1)),
            dma((2, copies - 1, units)),
            dma(()),
            pltpu.VMEM((mats, width), jnp.float32),
            pltpu.VMEM((height, slot_count), jnp.float32),
            dma((4,)),
        ]
        + [pltpu.VMEM((parts * slot_count, CHUNK, 128), jnp.bfloat16) for _ in range(units)],
        compiler_params=pltpu.CompilerParams(
            collective_id=0, has_side_effects=True, vmem_limit_bytes=63 * 2**20
        ),
        cost_estimate=pl.CostEstimate(flops=grad.size * 6, bytes_accessed=grad.size * 8, transcendentals=0),
        name="main",
    )(block_start, block_matrix, step, col_state, row_state.T, grad, param)

    landed = lax.ppermute(late, "dp", [(copies - 2, copies - 1), (1, 0)])
    size = total_blocks * copies * height * cut
    placed_shape = jax.ShapeDtypeStruct((total_blocks, copies, chunks, CHUNK, cut), jnp.bfloat16)
    new_cols, new_rows, placed = pl.pallas_call(
        functools.partial(place_kernel, tail),
        in_specs=[hbm, hbm, hbm, hbm],
        out_specs=[hbm, hbm, hbm],
        out_shape=[
            jax.ShapeDtypeStruct((mats, width), jnp.float32),
            jax.ShapeDtypeStruct((height, slot_count), jnp.float32),
            placed_shape,
        ],
        scratch_shapes=[
            pltpu.VMEM((mats, width), jnp.float32),
            pltpu.VMEM((height, slot_count), jnp.float32),
            dma((4,)),
            pltpu.VMEM((copies, chunks, total_blocks, CHUNK, cut), jnp.bfloat16),
            dma((copies, chunks)),
            dma((copies, chunks)),
            dma((copies, units)),
            dma((copies, units)),
            dma((tail,)),
            dma((tail,)),
        ],
        compiler_params=pltpu.CompilerParams(vmem_limit_bytes=60 * 2**20),
        cost_estimate=pl.CostEstimate(flops=size * 10, bytes_accessed=4 * size, transcendentals=0),
        name="place",
    )(new_cols, new_rows, temp, late)
    placed = pl.pallas_call(
        place_late_kernel,
        in_specs=[hbm, hbm],
        out_specs=hbm,
        out_shape=placed_shape,
        input_output_aliases={1: 0},
        scratch_shapes=[
            dma((tail,)),
        ],
        compiler_params=pltpu.CompilerParams(vmem_limit_bytes=4 * 2**20),
        cost_estimate=pl.CostEstimate(flops=size, bytes_accessed=size, transcendentals=0),
        name="place_late",
    )(landed, placed)
    new_params = placed.reshape(total_blocks * copies * height, cut)
    return new_params, new_rows.T, new_cols


def solution(mesh):
    return jax.shard_map(
        functools.partial(body, mesh.shape["shard"]),
        mesh=mesh,
        in_specs=(
            P("shard", "dp", None),
            P("shard", "dp", None),
            P("shard", "dp"),
            P(),
            P(),
            P(),
            P(),
        ),
        out_specs=(P(None, "shard"), P("shard", "dp"), P()),
        check_vma=False,
    )
```
